32 devices in a mesh: img: 16 (over z, x, core), band: 2 (over y).
Axes of the slice: x: 2, y: 2, z: 4, core: 2. Of those that a mesh axis runs over, the one named last changes fastest.
Arguments:
- block_input: bfloat16 [16384, 1152], P(('img', 'band')), may hold values from -6 to 6
- conditioning: bfloat16 [16, 1152], P('img'), may hold values from -6 to 6
- patch_valid: int32 [16384], P(('img', 'band')), may hold values from 0 to 1, as said below
- pos_rows: int32 [16384], P(('img', 'band')), may hold values from 0 to 31, as said below
- pos_cols: int32 [16384], P(('img', 'band')), may hold values from 0 to 63, as said below
- modulation_weight: bfloat16 [1152, 6, 1152], P(None, 'band'), may hold values from -0.1875 to 0.1875
- modulation_bias: bfloat16 [6, 1152], P('band'), may hold values from -3 to 3
- attend_weight: bfloat16 [1152, 3456], replicated, may hold values from -0.1875 to 0.1875
- query_bias: bfloat16 [1152], replicated, may hold values from -3 to 3
- value_bias: bfloat16 [1152], replicated, may hold values from -3 to 3
- project_weight: bfloat16 [1152, 1152], replicated, may hold values from -1 to 1
- project_bias: bfloat16 [1152], replicated, may hold values from -3 to 3
- expand_weight: bfloat16 [1152, 4608], replicated, may hold values from -0.1875 to 0.1875
- expand_bias: bfloat16 [4608], replicated, may hold values from -3 to 3
- contract_weight: bfloat16 [4608, 1152], replicated, may hold values from -0.1875 to 0.1875
- contract_bias: bfloat16 [1152], replicated, may hold values from -3 to 3
- out_cotangent: bfloat16 [16384, 1152], P(('img', 'band')), may hold values from -6 to 6
Outputs:
- block_output: bfloat16 [16384, 1152], P(('img', 'band'))
- input_grad: float32 [16384, 1152], P(('img', 'band'))
- conditioning_grad: float32 [16, 1152], P('img')
- modulation_weight_grad: float32 [1152, 6, 1152], P('img', 'band')
- modulation_bias_grad: float32 [6, 1152], P('band')
- attend_weight_grad: float32 [1152, 3456], P('img', 'band')
- query_bias_grad: float32 [1152], replicated
- value_bias_grad: float32 [1152], replicated
- project_weight_grad: float32 [1152, 1152], P('img', 'band')
- project_bias_grad: float32 [1152], replicated
- expand_weight_grad: float32 [1152, 4608], P('img', 'band')
- expand_bias_grad: float32 [4608], replicated
- contract_weight_grad: float32 [4608, 1152], P('img', 'band')
- contract_bias_grad: float32 [1152], replicated
The draws below stay inside these ranges and needn't reach their ends.
Inputs may be any that keep to these rules, and one draw needn't show every extreme that they name: `patch_valid`: slot s of a device belongs to the device's image s // 512. An image's grid is 16 x 2 * 32, 24 x 5 * 8 or 32 x 32 patches; band index 0 holds its upper half of rows and band index 1 its lower half, in row-major order in the first slots of the image's block, marked 1; the rest of the block is padding. `pos_rows`: the patch's row in its image's grid, 0 on padding slots. `pos_cols`: the patch's column in its image's grid, 0 on padding slots.
All inputs are finite; a program needn't handle non-finite values.
Results may differ from the reference program's by a relative error of at most 0.0147.
The reference program's roundings to bfloat16 on the way count: a program that leaves them out, or rounds other values in their place, can miss the bound.
Values may be sent and summed in bfloat16 or wider, within the bound.
A program may use at most 320 MiB of HBM per device.

```python
import math
import jax
import jax.numpy as jnp
from jax import lax

D = 1152
HEADS = 16
MLP = 4608
GRID_SIDE = 32
PATCH_SLOT = 512
IMG_DEV = 1
SLOTS = 512
IMAGES = 16
TOKENS = 16384
N_IMG = 16
N_BAND = 2


def grid_layout(key):
    grid_kinds = jax.random.randint(jax.random.fold_in(key, 11), (IMAGES,), 0, 3)
    grid_kinds = grid_kinds.at[0].set(1).at[1].set(2).at[2].set(0)
    row_index = jnp.arange(TOKENS, dtype=jnp.int32)
    device_index = row_index // SLOTS
    band_index = device_index % N_BAND
    image_index = device_index // N_BAND * IMG_DEV + row_index % SLOTS // PATCH_SLOT
    offset_slot = row_index % PATCH_SLOT
    own_kind = grid_kinds[image_index]
    grid_width = jnp.where(own_kind == 0, 2 * GRID_SIDE, jnp.where(own_kind == 1, 5 * GRID_SIDE // 4, GRID_SIDE))
    half_rows = jnp.where(own_kind == 0, GRID_SIDE // 4, jnp.where(own_kind == 1, 3 * GRID_SIDE // 8, GRID_SIDE // 2))
    is_patch = offset_slot < half_rows * grid_width
    grid_row = jnp.where(is_patch, band_index * half_rows + offset_slot // grid_width, 0)
    grid_col = jnp.where(is_patch, offset_slot % grid_width, 0)
    return (is_patch.astype(jnp.int32), grid_row.astype(jnp.int32), grid_col.astype(jnp.int32))


def draw_patch_valid(key, part):
    return grid_layout(key)[0]


def draw_pos_rows(key, part):
    return grid_layout(key)[1]


def draw_pos_cols(key, part):
    return grid_layout(key)[2]


def levels(own_key, extent, pieces, least, top_value):
    factor_of = 1.0
    for dim, blocks in pieces:
        steps = jax.random.uniform(jax.random.fold_in(jax.random.fold_in(own_key, 6), dim), (blocks,), jnp.float32, least / len(pieces), top_value / len(pieces))
        factor_of = factor_of * jnp.repeat(jnp.exp(steps), extent[dim] // blocks).reshape((-1,) + (1,) * (len(extent) - 1 - dim))
    return factor_of


def normal_values(rng, dims, width, limit, pieces=(), held_as=jnp.bfloat16):
    entries = width * jax.random.normal(rng, dims, jnp.float32)
    if pieces:
        entries = entries * levels(rng, dims, pieces, -0.22, 0.18)
    return jnp.clip(entries, -limit, limit).astype(held_as)


def setup_inputs(seed: int = 0) -> dict:
    splits = jax.random.split(jax.random.key(seed), 18)
    block_input = normal_values(splits[0], (TOKENS, D), 1.0, 6.0, ((0, 32),))
    conditioning = normal_values(splits[1], (IMAGES, D), 1.0, 6.0, ((0, 16),))
    patch_valid = draw_patch_valid(jax.random.fold_in(splits[17], 71), 0)
    pos_rows = draw_pos_rows(jax.random.fold_in(splits[17], 71), 0)
    pos_cols = draw_pos_cols(jax.random.fold_in(splits[17], 71), 0)
    modulation_weight = normal_values(splits[5], (D, 6, D), D ** -0.5, 0.1875, ((1, 2),))
    modulation_bias = normal_values(splits[6], (6, D), 0.3, 3.0, ((0, 2),))
    attend_weight = normal_values(splits[7], (D, 3 * D), D ** -0.5, 0.1875)
    query_bias = normal_values(splits[8], (D,), 0.5, 3.0)
    value_bias = normal_values(splits[9], (D,), 0.5, 3.0)
    project_weight = normal_values(splits[10], (D, D), (D // 32) ** -0.5, 1.0)
    project_bias = normal_values(splits[11], (D,), 0.5, 3.0)
    expand_weight = normal_values(splits[12], (D, MLP), D ** -0.5, 0.1875)
    expand_bias = normal_values(splits[13], (MLP,), 0.5, 3.0)
    contract_weight = normal_values(splits[14], (MLP, D), (MLP // 4) ** -0.5, 0.1875)
    contract_bias = normal_values(splits[15], (D,), 0.5, 3.0)
    out_cotangent = normal_values(splits[16], (TOKENS, D), 1.0, 6.0, ((0, 32),))
    return {"block_input": block_input, "conditioning": conditioning, "patch_valid": patch_valid, "pos_rows": pos_rows, "pos_cols": pos_cols, "modulation_weight": modulation_weight, "modulation_bias": modulation_bias, "attend_weight": attend_weight, "query_bias": query_bias, "value_bias": value_bias, "project_weight": project_weight, "project_bias": project_bias, "expand_weight": expand_weight, "expand_bias": expand_bias, "contract_weight": contract_weight, "contract_bias": contract_bias, "out_cotangent": out_cotangent}


@jax.custom_vjp
def low(v):
    return lax.optimization_barrier(v.astype(jnp.bfloat16)).astype(jnp.float32)

@jax.custom_vjp
def low_back(v):
    return v

def low_keep(v):
    return (low(v), None)

def low_pass(kept, grad):
    return (grad,)

def back_keep(v):
    return (v, None)

def back_low(kept, grad):
    return (low(grad),)
low.defvjp(low_keep, low_pass)
low_back.defvjp(back_keep, back_low)

def layer_norm(values):
    row_mean = lax.optimization_barrier(jnp.mean(values, axis=-1, keepdims=True))
    centred = values - row_mean
    spread = lax.optimization_barrier(jnp.mean(centred * centred, axis=-1, keepdims=True))
    return centred * lax.rsqrt(spread + 1e-06)

def gelu_tanh(values):
    return 0.5 * values * (1.0 + jnp.tanh(0.7978845608028654 * (values + 0.044715 * values * values * values)))

def swish_gate(values):
    return values / (1.0 + jnp.exp(-values))

def position_table(rows_in, cols_in, features):
    quarter = features // 4
    frequency = jnp.exp(-math.log(10000.0) * jnp.arange(quarter, dtype=jnp.float32) / quarter)
    col_angle = cols_in.astype(jnp.float32)[:, None] * frequency[None, :]
    row_angle = rows_in.astype(jnp.float32)[:, None] * frequency[None, :]
    return jnp.concatenate([jnp.sin(col_angle), jnp.cos(col_angle), jnp.sin(row_angle), jnp.cos(row_angle)], axis=1)

def group_forward(weights, token_rows, cond_rows, valid_rows, pos_table):
    modulation_weight, modulation_bias, attend_weight, query_bias, value_bias, project_weight, project_bias, expand_weight, expand_bias, contract_weight, contract_bias = weights
    highest = lax.Precision.HIGHEST
    head_size = D // HEADS
    score_scale = 1.0 / math.sqrt(head_size)
    activated = low(swish_gate(cond_rows))
    modulation = low_back(jnp.einsum('id,dkc->ikc', activated, modulation_weight, precision=highest) + modulation_bias)

    def modulate(values, shift_rows, scale_rows):
        return layer_norm(values) * (1.0 + scale_rows[None, :, None, :]) + shift_rows[None, :, None, :]
    hidden = (token_rows + pos_table).reshape(N_BAND, IMG_DEV, PATCH_SLOT, D)
    first_low = low(modulate(hidden, modulation[:, 0], modulation[:, 1])).reshape(-1, D)
    projected = jnp.dot(first_low, attend_weight, precision=highest)
    queries = low(low_back(projected[:, :D] + query_bias))
    key_rows = low(low_back(projected[:, D:2 * D]))
    value_rows = low(low_back(projected[:, 2 * D:] + value_bias))
    head_shape = (N_BAND, IMG_DEV, PATCH_SLOT, HEADS, head_size)
    query_heads = queries.reshape(head_shape)
    key_heads = key_rows.reshape(head_shape)
    value_heads = value_rows.reshape(head_shape)
    scores = low_back(jnp.einsum('biqhe,cikhe->ihbqck', query_heads, key_heads, precision=highest) * score_scale)
    key_mask = (valid_rows.reshape(N_BAND, IMG_DEV, PATCH_SLOT) > 0).transpose(1, 0, 2)[:, None, None, None, :, :]
    masked = jnp.where(key_mask, scores, -1e+30)
    row_top = lax.optimization_barrier(jnp.max(masked, axis=(4, 5), keepdims=True))
    exp_scores = jnp.exp(masked - row_top)
    probabilities = exp_scores / lax.optimization_barrier(jnp.sum(exp_scores, axis=(4, 5), keepdims=True))
    attended = jnp.einsum('ihbqck,cikhe->biqhe', low(probabilities), value_heads, precision=highest)
    mixed_low = low(low_back(attended.reshape(-1, D)))
    branch = low_back(jnp.dot(mixed_low, project_weight, precision=highest) + project_bias)
    middle = hidden + modulation[:, 2][None, :, None, :] * branch.reshape(N_BAND, IMG_DEV, PATCH_SLOT, D)
    second_low = low(modulate(middle, modulation[:, 3], modulation[:, 4])).reshape(-1, D)
    expanded = low_back(jnp.dot(second_low, expand_weight, precision=highest) + expand_bias)
    activation = low(gelu_tanh(expanded))
    mlp_out = low_back(jnp.dot(activation, contract_weight, precision=highest) + contract_bias)
    result = middle + modulation[:, 5][None, :, None, :] * mlp_out.reshape(N_BAND, IMG_DEV, PATCH_SLOT, D)
    return result.reshape(-1, D)

def reference(block_input, conditioning, patch_valid, pos_rows, pos_cols, modulation_weight, modulation_bias, attend_weight, query_bias, value_bias, project_weight, project_bias, expand_weight, expand_bias, contract_weight, contract_bias, out_cotangent):
    weights = tuple((member.astype(jnp.float32) for member in (modulation_weight, modulation_bias, attend_weight, query_bias, value_bias, project_weight, project_bias, expand_weight, expand_bias, contract_weight, contract_bias)))
    group_rows = N_BAND * SLOTS
    tables = position_table(pos_rows, pos_cols, D).reshape(N_IMG, group_rows, D)
    token_groups = block_input.astype(jnp.float32).reshape(N_IMG, group_rows, D)
    cond_groups = conditioning.astype(jnp.float32).reshape(N_IMG, IMG_DEV, D)
    valid_groups = patch_valid.reshape(N_IMG, group_rows)
    cot_groups = out_cotangent.astype(jnp.float32).reshape(N_IMG, group_rows, D)

    def group_step(running_sum, member):
        group_tokens, group_conds, group_valid, group_table, group_cot = member

        def forward(weight_set, tokens_in, conds_in):
            return group_forward(weight_set, tokens_in, conds_in, group_valid, group_table)
        result, backward = jax.vjp(forward, weights, group_tokens, group_conds)
        mask_rows = (group_valid > 0).astype(jnp.float32)[:, None]
        weight_grads, token_grads, cond_grads = backward(group_cot * mask_rows)
        running_sum = tuple((running + adding for running, adding in zip(running_sum, weight_grads)))
        return (running_sum, (result.astype(jnp.bfloat16), token_grads, cond_grads))
    zero_grads = tuple((jnp.zeros_like(member) for member in weights))
    totals, (outputs, token_grads, cond_grads) = lax.scan(group_step, zero_grads, (token_groups, cond_groups, valid_groups, tables, cot_groups))
    return (outputs.reshape(TOKENS, D), token_grads.reshape(TOKENS, D), cond_grads.reshape(IMAGES, D), totals[0], totals[1], totals[2], totals[3], totals[4], totals[5], totals[6], totals[7], totals[8], totals[9], totals[10])
```

```python
import math

import jax
import jax.numpy as jnp
from jax import lax
from jax.sharding import PartitionSpec as P

HEADS = 16


def layer_norm(values):
    row_mean = jnp.mean(values, axis=-1, keepdims=True)
    centred = values - row_mean
    spread = jnp.mean(centred * centred, axis=-1, keepdims=True)
    return centred * lax.rsqrt(spread + 1e-06)


def gelu_tanh(values):
    return (
        0.5
        * values
        * (1.0 + jnp.tanh(0.7978845608028654 * (values + 0.044715 * values * values * values)))
    )


def swish_gate(values):
    return values / (1.0 + jnp.exp(-values))


def position_table(rows_in, cols_in, features):
    quarter = features // 4
    frequency = jnp.exp(-math.log(10000.0) * jnp.arange(quarter, dtype=jnp.float32) / quarter)
    col_angle = cols_in.astype(jnp.float32)[:, None] * frequency[None, :]
    row_angle = rows_in.astype(jnp.float32)[:, None] * frequency[None, :]
    return jnp.concatenate(
        [jnp.sin(col_angle), jnp.cos(col_angle), jnp.sin(row_angle), jnp.cos(row_angle)], axis=1
    )


def norm_modulate(values, shift_rows, scale_rows):
    return layer_norm(values) * (1.0 + scale_rows[:, None, :]) + shift_rows[:, None, :]


def swap_bit(value, bit):
    members = lax.axis_size("img")
    return lax.ppermute(value, "img", [(i, i ^ (1 << bit)) for i in range(members)])


def swap_band(value):
    return lax.ppermute(value, "band", [(0, 1), (1, 0)])


def swap(value, stage):
    return swap_band(value) if stage == "band" else swap_bit(value, stage)


def my_bit(stage):
    if stage == "band":
        return lax.axis_index("band")
    return (lax.axis_index("img") >> stage) & 1


def pick(choice, if_zero, if_one):
    return jnp.where(choice == 0, if_zero, if_one)


def image_bits():
    return lax.axis_size("img").bit_length() - 1


def core_columns(values, core, band):
    quarter = values.shape[1] // 4
    pieces = [values[:, i * quarter : (i + 1) * quarter] for i in range(4)]
    return pick(
        band, pick(core, pieces[0], pieces[1]), pick(core, pieces[2], pieces[3])
    )


def weight_grad(left, right, order):
    bits = image_bits()
    core, band = my_bit(0), my_bit("band")
    left_all = jnp.concatenate([left, swap_bit(left, 0)], axis=0)
    quarter = right.shape[1] // 4
    kept_cols = jnp.concatenate(
        [core_columns(right, core, band), core_columns(right, core, 1 - band)], axis=1
    )
    sent_cols = jnp.concatenate(
        [core_columns(right, 1 - core, band), core_columns(right, 1 - core, 1 - band)], axis=1
    )
    right_all = jnp.concatenate([kept_cols, swap_bit(sent_cols, 0)], axis=0)
    row_shape = (2,) * (bits - 1) + (left.shape[1] >> (bits - 1), quarter)

    def product(columns):
        return (
            jnp.einsum("tk,tn->kn", left_all, columns, preferred_element_type=jnp.float32)
            .astype(jnp.bfloat16)
            .reshape(row_shape)
        )

    blocks = [product(right_all[:, quarter:]), product(right_all[:, :quarter])]
    alive = list(range(bits - 1, 0, -1))
    for stage in order:
        if stage == "band":
            other, mine = blocks
            blocks = [mine.astype(jnp.float32) + swap_band(other).astype(jnp.float32)]
        else:
            axis = alive.index(stage)
            alive.remove(stage)
            side = my_bit(stage)

            def halve(block):
                going = lax.dynamic_index_in_dim(block, 1 - side, axis, keepdims=False)
                staying = lax.dynamic_index_in_dim(block, side, axis, keepdims=False)
                return staying.astype(jnp.float32) + swap_bit(
                    going.astype(jnp.bfloat16), stage
                ).astype(jnp.float32)

            blocks = [halve(block) for block in blocks]
        if stage != order[-1]:
            blocks = [block.astype(jnp.bfloat16) for block in blocks]
    total = blocks[0]
    rows = total.shape[0] // 2
    low, high = total[:rows], total[rows:]
    here, there = pick(core, low, high), swap_bit(pick(core, high, low), 0)
    return pick(
        core,
        jnp.concatenate([here, there], axis=1),
        jnp.concatenate([there, here], axis=1),
    )


def sum_all(value):
    for stage in ["band"] + list(range(image_bits())):
        value = value + swap(value, stage)
    return value


def gather_images(value):
    for stage in range(image_bits()):
        other = swap_bit(value, stage)
        side = my_bit(stage)
        value = jnp.concatenate([pick(side, value, other), pick(side, other, value)], axis=0)
    return value


def shards(
    block_input,
    conditioning,
    patch_valid,
    pos_rows,
    pos_cols,
    modulation_weight,
    modulation_bias,
    attend_weight,
    query_bias,
    value_bias,
    project_weight,
    project_bias,
    expand_weight,
    expand_bias,
    contract_weight,
    contract_bias,
    out_cotangent,
):
    slot_count, features = block_input.shape
    image_count = conditioning.shape[0]
    per_image = slot_count // image_count
    head_count = HEADS
    rest = list(range(2, image_bits()))
    y_first = ["band", 1] + rest
    x_first = [1] + rest + ["band"]
    z_first = rest + ["band", 1]
    head_size = features // head_count
    score_scale = 1.0 / math.sqrt(head_size)
    valid_rows = patch_valid.astype(jnp.float32)
    band = lax.axis_index("band")
    other_input = swap_band(block_input)
    places = jnp.stack([pos_rows, pos_cols, patch_valid])
    other_places = swap_band(places)
    pos_table = position_table(pos_rows, pos_cols, features)
    other_table = position_table(other_places[0], other_places[1], features)
    hidden = block_input.astype(jnp.float32) + pos_table
    shaped = hidden.reshape(image_count, per_image, features)
    cond_float = conditioning.astype(jnp.float32)
    swish_value, swish_back = jax.vjp(swish_gate, cond_float)
    activated = swish_value.astype(jnp.bfloat16)
    modulation_half = jnp.einsum(
        "id,dkc->ikc", activated, modulation_weight, preferred_element_type=jnp.float32
    ) + modulation_bias.astype(jnp.float32)
    modulation_other = swap_band(modulation_half)
    modulation = jnp.concatenate(
        [
            pick(band, modulation_half, modulation_other),
            pick(band, modulation_other, modulation_half),
        ],
        axis=1,
    )
    shift_one, scale_one, gate_one = (modulation[:, 0], modulation[:, 1], modulation[:, 2])
    shift_two, scale_two, gate_two = (modulation[:, 3], modulation[:, 4], modulation[:, 5])
    first_mod, first_back = jax.vjp(norm_modulate, shaped, shift_one, scale_one)
    first_low = first_mod.astype(jnp.bfloat16).reshape(slot_count, features)
    projected = jnp.dot(first_low, attend_weight, preferred_element_type=jnp.float32)
    queries = (projected[:, :features] + query_bias.astype(jnp.float32)).astype(jnp.bfloat16)
    other_shaped = (other_input.astype(jnp.float32) + other_table).reshape(
        image_count, per_image, features
    )
    other_low = (
        norm_modulate(other_shaped, shift_one, scale_one)
        .astype(jnp.bfloat16)
        .reshape(slot_count, features)
    )
    other_projected = jnp.dot(
        other_low, attend_weight[:, features:], preferred_element_type=jnp.float32
    )

    def key_value(key_part, value_part):
        return (
            key_part.astype(jnp.bfloat16),
            (value_part + value_bias.astype(jnp.float32)).astype(jnp.bfloat16),
        )

    keys_own, values_own = key_value(
        projected[:, features : 2 * features], projected[:, 2 * features :]
    )
    keys_other, values_other = key_value(
        other_projected[:, :features], other_projected[:, features:]
    )
    keys_all = jnp.concatenate([keys_own, keys_other], axis=0)
    values_all = jnp.concatenate([values_own, values_other], axis=0)
    valid_all = jnp.concatenate([patch_valid, other_places[2]], axis=0)
    band_count = 2
    head_shape = (band_count, image_count, per_image, head_count, head_size)
    query_heads = queries.reshape(image_count, per_image, head_count, head_size)
    key_mask = (valid_all.reshape(band_count, image_count, per_image).transpose(1, 0, 2) > 0)[
        :, None, None, :, :
    ]

    def score_block(key_block):
        key_heads = key_block.reshape(head_shape)
        raw_scores = (
            jnp.einsum(
                "iqhe,bikhe->ihqbk", query_heads, key_heads, preferred_element_type=jnp.float32
            )
            * score_scale
        )
        return jnp.where(key_mask, raw_scores, -1e30)

    scores = score_block(keys_all)
    row_top = jnp.max(scores, axis=(3, 4), keepdims=True)
    row_total = jnp.sum(jnp.exp(scores - row_top), axis=(3, 4), keepdims=True)
    log_total = row_top + jnp.log(row_total)
    probabilities = jnp.exp(scores - log_total).astype(jnp.bfloat16)
    attended = jnp.einsum(
        "ihqbk,bikhe->iqhe",
        probabilities,
        values_all.reshape(head_shape),
        preferred_element_type=jnp.float32,
    )
    mixed_low = attended.reshape(slot_count, features).astype(jnp.bfloat16)
    branch = jnp.dot(
        mixed_low, project_weight, preferred_element_type=jnp.float32
    ) + project_bias.astype(jnp.float32)
    branch_rows = branch.reshape(image_count, per_image, features)
    middle = shaped + gate_one[:, None, :] * branch_rows
    second_mod, second_back = jax.vjp(norm_modulate, middle, shift_two, scale_two)
    second_low = second_mod.astype(jnp.bfloat16).reshape(slot_count, features)
    expanded = jnp.dot(
        second_low, expand_weight, preferred_element_type=jnp.float32
    ) + expand_bias.astype(jnp.float32)
    activation, gelu_back = jax.vjp(gelu_tanh, expanded)
    activation_low = activation.astype(jnp.bfloat16)
    mlp_out = jnp.dot(
        activation_low, contract_weight, preferred_element_type=jnp.float32
    ) + contract_bias.astype(jnp.float32)
    mlp_rows = mlp_out.reshape(image_count, per_image, features)
    result = middle + gate_two[:, None, :] * mlp_rows
    block_output = result.reshape(slot_count, features).astype(jnp.bfloat16)
    upstream = (out_cotangent.astype(jnp.float32) * valid_rows[:, None]).reshape(
        image_count, per_image, features
    )
    grad_gate_two = jnp.sum(upstream * mlp_rows, axis=1)
    grad_mlp = (gate_two[:, None, :] * upstream).reshape(slot_count, features).astype(jnp.bfloat16)
    contract_out = weight_grad(activation_low, grad_mlp, x_first)
    contract_bias_grad = jnp.sum(grad_mlp.astype(jnp.float32), axis=0)
    grad_activation = jnp.einsum(
        "td,fd->tf", grad_mlp, contract_weight, preferred_element_type=jnp.float32
    )
    grad_expanded = gelu_back(grad_activation)[0].astype(jnp.bfloat16)
    expand_out = weight_grad(second_low, grad_expanded, y_first)
    expand_bias_grad = jnp.sum(grad_expanded.astype(jnp.float32), axis=0)
    grad_second = jnp.einsum(
        "tf,df->td", grad_expanded, expand_weight, preferred_element_type=jnp.float32
    )
    grad_norm_two, grad_shift_two, grad_scale_two = second_back(
        grad_second.reshape(image_count, per_image, features)
    )
    grad_middle = upstream + grad_norm_two
    grad_gate_one = jnp.sum(grad_middle * branch_rows, axis=1)
    grad_branch = (
        (gate_one[:, None, :] * grad_middle).reshape(slot_count, features).astype(jnp.bfloat16)
    )
    project_out = weight_grad(mixed_low, grad_branch, z_first)
    project_bias_grad = jnp.sum(grad_branch.astype(jnp.float32), axis=0)
    grad_mixed = jnp.einsum(
        "td,ed->te", grad_branch, project_weight, preferred_element_type=jnp.float32
    ).astype(jnp.bfloat16)
    grad_heads = grad_mixed.reshape(image_count, per_image, head_count, head_size)
    keys_back, values_back = keys_all, values_all
    scores_back = score_block(keys_back)
    probs_back = jnp.exp(scores_back - log_total)
    grad_probs = jnp.einsum(
        "iqhe,bikhe->ihqbk",
        grad_heads,
        values_back.reshape(head_shape),
        preferred_element_type=jnp.float32,
    )
    row_delta = jnp.sum(probs_back * grad_probs, axis=(3, 4), keepdims=True)
    grad_scores = (probs_back * (grad_probs - row_delta)).astype(jnp.bfloat16)
    grad_query = (
        jnp.einsum(
            "ihqbk,bikhe->iqhe",
            grad_scores,
            keys_back.reshape(head_shape),
            preferred_element_type=jnp.float32,
        )
        * score_scale
    )
    grad_key_part = (
        jnp.einsum(
            "ihqbk,iqhe->bikhe", grad_scores, query_heads, preferred_element_type=jnp.float32
        )
        * score_scale
    )
    grad_value_part = jnp.einsum(
        "ihqbk,iqhe->bikhe",
        probs_back.astype(jnp.bfloat16),
        grad_heads,
        preferred_element_type=jnp.float32,
    )
    def own_total(part):
        halves = part.reshape(band_count, slot_count, features)
        return halves[0] + swap_band(halves[1].astype(jnp.bfloat16)).astype(jnp.float32)

    grad_key, grad_value = own_total(grad_key_part), own_total(grad_value_part)
    grad_qkv = jnp.concatenate(
        [grad_query.reshape(slot_count, features), grad_key, grad_value], axis=1
    ).astype(jnp.bfloat16)
    attend_out = weight_grad(first_low, grad_qkv, z_first)
    query_bias_grad = jnp.sum(grad_qkv[:, :features].astype(jnp.float32), axis=0)
    value_bias_grad = jnp.sum(grad_qkv[:, 2 * features :].astype(jnp.float32), axis=0)
    grad_first = jnp.einsum(
        "te,de->td", grad_qkv, attend_weight, preferred_element_type=jnp.float32
    )
    grad_norm_one, grad_shift_one, grad_scale_one = first_back(
        grad_first.reshape(image_count, per_image, features)
    )
    input_grad = (grad_middle + grad_norm_one).reshape(slot_count, features)
    grad_modulation = jnp.stack(
        [
            grad_shift_one,
            grad_scale_one,
            grad_gate_one,
            grad_shift_two,
            grad_scale_two,
            grad_gate_two,
        ],
        axis=1,
    )
    grad_halves = grad_modulation.reshape(image_count, 2, -1, features)
    modulation_grad_half = (
        pick(band, grad_halves[:, 0], grad_halves[:, 1])
        + swap_band(pick(band, grad_halves[:, 1], grad_halves[:, 0]))
    ).astype(jnp.bfloat16)
    activated_grad_part = jnp.einsum(
        "ikc,dkc->id", modulation_grad_half, modulation_weight, preferred_element_type=jnp.float32
    )
    conditioning_grad = swish_back(activated_grad_part + swap_band(activated_grad_part))[0]
    all_grads = gather_images(modulation_grad_half)
    all_activated = gather_images(activated)
    block_rows = features // lax.axis_size("img")
    own_activated = lax.dynamic_slice_in_dim(
        all_activated, lax.axis_index("img") * block_rows, block_rows, axis=1
    )
    modulation_grad_out = jnp.einsum(
        "id,ikc->dkc", own_activated, all_grads, preferred_element_type=jnp.float32
    )
    modulation_bias_out = jnp.sum(all_grads.astype(jnp.float32), axis=0)
    bias_parts = [
        query_bias_grad,
        value_bias_grad,
        project_bias_grad,
        expand_bias_grad,
        contract_bias_grad,
    ]
    bias_total = sum_all(jnp.concatenate(bias_parts))
    bias_outs = []
    place = 0
    for part in bias_parts:
        bias_outs.append(bias_total[place : place + part.shape[0]])
        place += part.shape[0]
    (
        query_bias_out,
        value_bias_out,
        project_bias_out,
        expand_bias_out,
        contract_bias_out,
    ) = bias_outs
    return (
        block_output,
        input_grad,
        conditioning_grad,
        modulation_grad_out,
        modulation_bias_out,
        attend_out,
        query_bias_out,
        value_bias_out,
        project_out,
        project_bias_out,
        expand_out,
        expand_bias_out,
        contract_out,
        contract_bias_out,
    )


def solution(mesh):
    in_specs = (
        P(("img", "band"), None),
        P("img", None),
        P(("img", "band")),
        P(("img", "band")),
        P(("img", "band")),
        P(None, "band", None),
        P("band", None),
        P(),
        P(),
        P(),
        P(),
        P(),
        P(),
        P(),
        P(),
        P(),
        P(("img", "band"), None),
    )
    out_specs = (
        P(("img", "band"), None),
        P(("img", "band"), None),
        P("img", None),
        P("img", "band", None),
        P("band", None),
        P("img", "band"),
        P(),
        P(),
        P("img", "band"),
        P(),
        P("img", "band"),
        P(),
        P("img", "band"),
        P(),
    )
    return jax.shard_map(shards, mesh=mesh, in_specs=in_specs, out_specs=out_specs, check_vma=False)
```

```python
import functools
import math

import jax
import jax.numpy as jnp
from jax import lax
from jax.experimental import pallas as pl
from jax.sharding import PartitionSpec as P

HEADS = 16


def layer_norm(values):
    row_mean = jnp.mean(values, axis=-1, keepdims=True)
    centred = values - row_mean
    spread = jnp.mean(centred * centred, axis=-1, keepdims=True)
    return centred * lax.rsqrt(spread + 1e-06)


def gelu_tanh(values):
    return (
        0.5
        * values
        * (1.0 + jnp.tanh(0.7978845608028654 * (values + 0.044715 * values * values * values)))
    )


def swish_gate(values):
    return values / (1.0 + jnp.exp(-values))


ROW_PLACES, COL_PLACES = 32, 64


def position_pieces(features):
    quarter = features // 4
    frequency = jnp.exp(-math.log(10000.0) * jnp.arange(quarter, dtype=jnp.float32) / quarter)
    angle = jnp.arange(COL_PLACES, dtype=jnp.float32)[:, None] * frequency[None, :]
    waves = jnp.concatenate([jnp.sin(angle), jnp.cos(angle)], axis=1)
    pieces = []
    for _ in range(3):
        piece = lax.reduce_precision(waves, 8, 7)
        pieces.append(piece.astype(jnp.bfloat16))
        waves = waves - piece
    blank = jnp.zeros_like(pieces[0])
    return jnp.concatenate(
        [jnp.concatenate([piece, blank], axis=1) for piece in pieces]
        + [jnp.concatenate([blank, piece], axis=1)[:ROW_PLACES] for piece in pieces],
        axis=0,
    )


def position_table(rows_in, cols_in, pieces):
    spot = jnp.arange(pieces.shape[0])[None, :]
    col_spots = 3 * COL_PLACES
    chosen = jnp.where(
        spot < col_spots,
        spot % COL_PLACES == cols_in[:, None],
        (spot - col_spots) % ROW_PLACES == rows_in[:, None],
    )
    return jnp.dot(chosen.astype(jnp.bfloat16), pieces, preferred_element_type=jnp.float32)


def norm_modulate(values, shift_rows, scale_rows):
    return layer_norm(values) * (1.0 + scale_rows[:, None, :]) + shift_rows[:, None, :]


def swap_bit(value, bit):
    members = lax.axis_size("img")
    return lax.ppermute(value, "img", [(i, i ^ (1 << bit)) for i in range(members)])


def swap_band(value):
    return lax.ppermute(value, "band", [(0, 1), (1, 0)])


def swap(value, stage):
    return swap_band(value) if stage == "band" else swap_bit(value, stage)


def my_bit(stage):
    if stage == "band":
        return lax.axis_index("band")
    return (lax.axis_index("img") >> stage) & 1


def pick(choice, if_zero, if_one):
    return jnp.where(choice == 0, if_zero, if_one)


def image_bits():
    return lax.axis_size("img").bit_length() - 1


def attend_kernel(score_scale, q_ref, k_ref, v_ref, kx_ref, vx_ref, mask_ref, out_ref, log_ref):
    keys = jnp.concatenate([k_ref[0], kx_ref[0]], axis=1)
    values = jnp.concatenate([v_ref[0], vx_ref[0]], axis=1)
    scores = lax.dot_general(
        keys, q_ref[0], (((0,), (0,)), ((), ())), preferred_element_type=jnp.float32
    )
    scores = jnp.where(mask_ref[...] > 0, scores * score_scale, -1e30)
    top = jnp.max(scores, axis=0, keepdims=True)
    weights = jnp.exp(scores - top)
    total = jnp.sum(weights, axis=0, keepdims=True)
    probabilities = (weights * (1.0 / total)).astype(jnp.bfloat16)
    out_ref[0] = jnp.dot(values, probabilities, preferred_element_type=jnp.float32).astype(
        jnp.bfloat16
    )
    log_ref[0] = top + jnp.log(total)


def head_blocks(size, rows, heads):
    block = lambda base: pl.BlockSpec((1, size, rows), lambda h: (base * heads + h, 0, 0))
    return [block(0), block(1), block(2), block(0), block(1)]


def attend_forward(own, other, mask, score_scale):
    heads, (_, size, rows) = HEADS, own.shape
    columns = 2 * rows
    return pl.pallas_call(
        functools.partial(attend_kernel, score_scale),
        grid=(heads,),
        in_specs=head_blocks(size, rows, heads)
        + [pl.BlockSpec((columns, 1), lambda h: (0, 0))],
        out_specs=[
            pl.BlockSpec((1, size, rows), lambda h: (h, 0, 0)),
            pl.BlockSpec((1, 1, rows), lambda h: (h, 0, 0)),
        ],
        out_shape=[
            jax.ShapeDtypeStruct((heads, size, rows), jnp.bfloat16),
            jax.ShapeDtypeStruct((heads, 1, rows), jnp.float32),
        ],
        cost_estimate=pl.CostEstimate(
            flops=16 * heads * 128 * rows * columns,
            bytes_accessed=4 * heads * size * (rows + columns),
            transcendentals=heads * rows * columns,
        ),
    )(own, own, own, other, other, mask)


def attend_back_kernel(
    score_scale,
    q_ref,
    k_ref,
    v_ref,
    kx_ref,
    vx_ref,
    go_ref,
    log_ref,
    mask_ref,
    dq_ref,
    own_ref,
    other_ref,
):
    queries, grads = q_ref[0], go_ref[0]
    keys = jnp.concatenate([k_ref[0], kx_ref[0]], axis=1)
    values = jnp.concatenate([v_ref[0], vx_ref[0]], axis=1)
    rows = queries.shape[1]

    def outer(left, right):
        return lax.dot_general(
            left, right, (((0,), (0,)), ((), ())), preferred_element_type=jnp.float32
        )

    def across(left, right):
        return lax.dot_general(
            left, right, (((1,), (1,)), ((), ())), preferred_element_type=jnp.float32
        )

    scores = jnp.where(mask_ref[...] > 0, outer(keys, queries) * score_scale, -1e30)
    weights = jnp.exp(scores - log_ref[0])
    grad_weights = outer(values, grads)
    delta = jnp.sum(weights * grad_weights, axis=0, keepdims=True)
    grad_scores = (weights * (grad_weights - delta)).astype(jnp.bfloat16)
    grad_values = across(grads, weights.astype(jnp.bfloat16))
    grad_keys = across(queries, grad_scores) * score_scale
    for i, grad in enumerate((grad_keys, grad_values)):
        own_ref[i, 0] = grad[:, :rows]
        other_ref[i, 0] = grad[:, rows:].astype(other_ref.dtype)
    dq_ref[0] = (
        jnp.dot(keys, grad_scores, preferred_element_type=jnp.float32) * score_scale
    ).astype(dq_ref.dtype)


def attend_backward(own, other, grads, log_total, mask, score_scale):
    heads, (_, size, rows) = HEADS, own.shape
    columns = 2 * rows
    single = pl.BlockSpec((1, size, rows), lambda h: (h, 0, 0))
    double = pl.BlockSpec((2, 1, size, rows), lambda h: (0, h, 0, 0))
    return pl.pallas_call(
        functools.partial(attend_back_kernel, score_scale),
        grid=(heads,),
        in_specs=head_blocks(size, rows, heads)
        + [
            single,
            pl.BlockSpec((1, 1, rows), lambda h: (h, 0, 0)),
            pl.BlockSpec((columns, 1), lambda h: (0, 0)),
        ],
        out_specs=[single, double, double],
        out_shape=[
            jax.ShapeDtypeStruct((heads, size, rows), jnp.bfloat16),
            jax.ShapeDtypeStruct((2, heads, size, rows), jnp.float32),
            jax.ShapeDtypeStruct((2, heads, size, rows), jnp.bfloat16),
        ],
        cost_estimate=pl.CostEstimate(
            flops=30 * heads * 128 * rows * columns,
            bytes_accessed=8 * heads * size * (rows + columns),
            transcendentals=heads * rows * columns,
        ),
    )(own, own, own, other, other, grads, log_total, mask)


def product_kernel(left_axis, right_axis, left_ref, left_far, right_ref, right_far, out_ref):
    contract = (((left_axis,), (right_axis,)), ((), ()))
    near = lax.dot_general(
        left_ref[...], right_ref[0], contract, preferred_element_type=jnp.float32
    )
    far = lax.dot_general(
        left_far[...], right_far[0], contract, preferred_element_type=jnp.float32
    )
    out_ref[0] = (near + far).astype(out_ref.dtype)


def row_product(left, left_far, right, right_far, left_axis, right_axis):
    depth, width = left.shape[left_axis], left.shape[1 - left_axis]
    columns = right.shape[2 - right_axis]
    tile = 384 if width % 384 == 0 else width
    left_block = (
        pl.BlockSpec((depth, tile), lambda b, k: (0, k))
        if left_axis == 0
        else pl.BlockSpec((tile, depth), lambda b, k: (k, 0))
    )
    right_block = pl.BlockSpec((1,) + right.shape[1:], lambda b, k: (b, 0, 0))
    return pl.pallas_call(
        functools.partial(product_kernel, left_axis, right_axis),
        grid=(2, width // tile),
        in_specs=[left_block, left_block, right_block, right_block],
        out_specs=pl.BlockSpec((1, tile, columns), lambda b, k: (b, k, 0)),
        out_shape=jax.ShapeDtypeStruct((2, width, columns), jnp.bfloat16),
        cost_estimate=pl.CostEstimate(
            flops=8 * depth * width * columns,
            bytes_accessed=8 * depth * (width + columns) + 4 * width * columns,
            transcendentals=0,
        ),
    )(left, left_far, right, right_far)


def core_columns(values, axis, core, band):
    quarter = values.shape[axis] // 4
    pieces = [lax.slice_in_dim(values, i * quarter, (i + 1) * quarter, axis=axis) for i in range(4)]
    return pick(
        band, pick(core, pieces[0], pieces[1]), pick(core, pieces[2], pieces[3])
    )


def chip_product(left, right, left_axis=0, right_axis=0):
    core, band = my_bit(0), my_bit("band")

    def columns(which):
        return jnp.stack(
            [core_columns(right, 1 - right_axis, which, b) for b in (1 - band, band)]
        )

    left_far, right_far = swap_bit(left, 0), swap_bit(columns(1 - core), 0)
    return row_product(left, left_far, columns(core), right_far, left_axis, right_axis)


def scatter_sum(product, orders):
    bits = image_bits()
    core = my_bit(0)
    chunk = product.shape[1] >> (bits - 1)
    block = product.reshape((2,) * bits + (chunk, product.shape[2]))
    part = chunk // len(orders)
    totals = [
        scatter_part(block[..., i * part : (i + 1) * part, :], order)
        for i, order in enumerate(orders)
    ]
    total = jnp.concatenate(totals, axis=0) if len(totals) > 1 else totals[0]
    rows = chunk // 2
    low, high = total[:rows], total[rows:]
    here, there = pick(core, low, high), swap_bit(pick(core, high, low), 0)
    return pick(
        core,
        jnp.concatenate([here, there], axis=1),
        jnp.concatenate([there, here], axis=1),
    )


def scatter_part(block, order):
    alive = ["band"] + list(range(image_bits() - 1, 0, -1))
    for stage in order:
        axis = alive.index(stage)
        alive.remove(stage)
        first = lax.index_in_dim(block, 0, axis, keepdims=False)
        second = lax.index_in_dim(block, 1, axis, keepdims=False)
        if stage == "band":
            going, staying = first, second
        else:
            side = my_bit(stage)
            going, staying = pick(side, second, first), pick(side, first, second)
        block = staying.astype(jnp.float32) + swap(going, stage).astype(jnp.float32)
        if stage != order[-1]:
            block = block.astype(jnp.bfloat16)
    return block


def sum_all(value):
    for stage in ["band"] + list(range(image_bits())):
        value = value + swap(value, stage)
    return value


def gather_images(value):
    for stage in range(image_bits()):
        other = swap_bit(value, stage)
        side = my_bit(stage)
        value = jnp.concatenate([pick(side, value, other), pick(side, other, value)], axis=0)
    return value


def shards(
    block_input,
    conditioning,
    patch_valid,
    pos_rows,
    pos_cols,
    modulation_weight,
    modulation_bias,
    attend_weight,
    query_bias,
    value_bias,
    project_weight,
    project_bias,
    expand_weight,
    expand_bias,
    contract_weight,
    contract_bias,
    out_cotangent,
):
    slot_count, features = block_input.shape
    image_count = conditioning.shape[0]
    per_image = slot_count // image_count
    head_count = HEADS
    rest = list(range(2, image_bits()))
    y_first = ["band", 1] + rest
    x_first = [1] + rest + ["band"]
    z_first = rest + ["band", 1]
    head_size = features // head_count
    score_scale = 1.0 / math.sqrt(head_size)
    valid_rows = patch_valid.astype(jnp.float32)
    band = lax.axis_index("band")
    other_input = swap_band(block_input)
    places = jnp.stack([pos_rows, pos_cols, patch_valid])
    other_places = swap_band(places)
    pieces = position_pieces(features)
    pos_table = position_table(pos_rows, pos_cols, pieces)
    other_table = position_table(other_places[0], other_places[1], pieces)
    hidden = block_input.astype(jnp.float32) + pos_table
    shaped = hidden.reshape(image_count, per_image, features)
    cond_float = conditioning.astype(jnp.float32)
    swish_value, swish_back = jax.vjp(swish_gate, cond_float)
    activated = swish_value.astype(jnp.bfloat16)
    modulation_half = jnp.einsum(
        "id,dkc->ikc", activated, modulation_weight, preferred_element_type=jnp.float32
    ) + modulation_bias.astype(jnp.float32)
    modulation_other = swap_band(modulation_half)
    modulation = jnp.concatenate(
        [
            pick(band, modulation_half, modulation_other),
            pick(band, modulation_other, modulation_half),
        ],
        axis=1,
    )
    shift_one, scale_one, gate_one = (modulation[:, 0], modulation[:, 1], modulation[:, 2])
    shift_two, scale_two, gate_two = (modulation[:, 3], modulation[:, 4], modulation[:, 5])
    first_mod, first_back = jax.vjp(norm_modulate, shaped, shift_one, scale_one)
    first_low = first_mod.astype(jnp.bfloat16).reshape(slot_count, features)
    input_bias = jnp.concatenate(
        [query_bias, jnp.zeros_like(query_bias), value_bias]
    ).astype(jnp.float32)[:, None]

    def project_heads(rows, skip):
        flat = jnp.einsum(
            "dn,td->nt", attend_weight[:, skip:], rows, preferred_element_type=jnp.float32
        )
        return (flat + input_bias[skip:]).astype(jnp.bfloat16).reshape(-1, head_size, slot_count)

    own_heads = project_heads(first_low, 0)
    other_shaped = (other_input.astype(jnp.float32) + other_table).reshape(
        image_count, per_image, features
    )
    other_low = (
        norm_modulate(other_shaped, shift_one, scale_one)
        .astype(jnp.bfloat16)
        .reshape(slot_count, features)
    )
    other_heads = project_heads(other_low, features)
    key_mask = jnp.concatenate([patch_valid, other_places[2]]).astype(jnp.float32)[:, None]
    mixed_heads, log_total = attend_forward(own_heads, other_heads, key_mask, score_scale)
    mixed_low = mixed_heads.reshape(features, slot_count)
    branch = jnp.einsum(
        "et,ed->td", mixed_low, project_weight, preferred_element_type=jnp.float32
    ) + project_bias.astype(jnp.float32)
    branch_rows = branch.reshape(image_count, per_image, features)
    middle = shaped + gate_one[:, None, :] * branch_rows
    second_mod, second_back = jax.vjp(norm_modulate, middle, shift_two, scale_two)
    second_low = second_mod.astype(jnp.bfloat16).reshape(slot_count, features)
    expanded = jnp.dot(
        second_low, expand_weight, preferred_element_type=jnp.float32
    ) + expand_bias.astype(jnp.float32)
    activation, gelu_back = jax.vjp(gelu_tanh, expanded)
    activation_low = activation.astype(jnp.bfloat16)
    mlp_out = jnp.dot(
        activation_low, contract_weight, preferred_element_type=jnp.float32
    ) + contract_bias.astype(jnp.float32)
    mlp_rows = mlp_out.reshape(image_count, per_image, features)
    result = middle + gate_two[:, None, :] * mlp_rows
    block_output = result.reshape(slot_count, features).astype(jnp.bfloat16)
    upstream = (out_cotangent.astype(jnp.float32) * valid_rows[:, None]).reshape(
        image_count, per_image, features
    )
    grad_gate_two = jnp.sum(upstream * mlp_rows, axis=1)
    grad_mlp = (gate_two[:, None, :] * upstream).reshape(slot_count, features).astype(jnp.bfloat16)
    contract_chip = chip_product(activation_low, grad_mlp)
    contract_bias_grad = jnp.sum(grad_mlp.astype(jnp.float32), axis=0)
    grad_activation = jnp.einsum(
        "td,fd->tf", grad_mlp, contract_weight, preferred_element_type=jnp.float32
    )
    grad_expanded = gelu_back(grad_activation)[0].astype(jnp.bfloat16)
    expand_chip = chip_product(second_low, grad_expanded)
    expand_bias_grad = jnp.sum(grad_expanded.astype(jnp.float32), axis=0)
    grad_second = jnp.einsum(
        "tf,df->td", grad_expanded, expand_weight, preferred_element_type=jnp.float32
    )
    grad_norm_two, grad_shift_two, grad_scale_two = second_back(
        grad_second.reshape(image_count, per_image, features)
    )
    grad_middle = upstream + grad_norm_two
    grad_gate_one = jnp.sum(grad_middle * branch_rows, axis=1)
    grad_branch = (
        (gate_one[:, None, :] * grad_middle).reshape(slot_count, features).astype(jnp.bfloat16)
    )
    grad_branch, contract_chip, expand_chip = lax.optimization_barrier(
        (grad_branch, contract_chip, expand_chip)
    )
    contract_out = scatter_sum(contract_chip, [x_first])
    expand_out = scatter_sum(expand_chip, [y_first])
    project_out = scatter_sum(chip_product(mixed_low, grad_branch, left_axis=1), [z_first])
    project_bias_grad = jnp.sum(grad_branch.astype(jnp.float32), axis=0)
    grad_mixed = jnp.einsum(
        "td,ed->et", grad_branch, project_weight, preferred_element_type=jnp.float32
    ).astype(jnp.bfloat16)
    grad_query, grad_pair, grad_pair_other = attend_backward(
        own_heads,
        other_heads,
        grad_mixed.reshape(head_count, head_size, slot_count),
        log_total,
        key_mask,
        score_scale,
    )
    grad_pair = grad_pair + swap_band(grad_pair_other).astype(jnp.float32)
    grad_qkv = jnp.concatenate(
        [
            grad_query.reshape(features, slot_count),
            grad_pair.astype(jnp.bfloat16).reshape(2 * features, slot_count),
        ],
        axis=0,
    )
    attend_out = scatter_sum(
        chip_product(first_low, grad_qkv, right_axis=1), [x_first, y_first, z_first]
    )
    query_bias_grad = jnp.sum(grad_qkv[:features].astype(jnp.float32), axis=1)
    value_bias_grad = jnp.sum(grad_qkv[2 * features :].astype(jnp.float32), axis=1)
    grad_first = jnp.einsum(
        "et,de->td", grad_qkv, attend_weight, preferred_element_type=jnp.float32
    )
    grad_norm_one, grad_shift_one, grad_scale_one = first_back(
        grad_first.reshape(image_count, per_image, features)
    )
    input_grad = (grad_middle + grad_norm_one).reshape(slot_count, features)
    grad_modulation = jnp.stack(
        [
            grad_shift_one,
            grad_scale_one,
            grad_gate_one,
            grad_shift_two,
            grad_scale_two,
            grad_gate_two,
        ],
        axis=1,
    )
    grad_halves = grad_modulation.reshape(image_count, 2, -1, features)
    modulation_grad_half = (
        pick(band, grad_halves[:, 0], grad_halves[:, 1])
        + swap_band(pick(band, grad_halves[:, 1], grad_halves[:, 0]))
    ).astype(jnp.bfloat16)
    activated_grad_part = jnp.einsum(
        "ikc,dkc->id", modulation_grad_half, modulation_weight, preferred_element_type=jnp.float32
    )
    conditioning_grad = swish_back(activated_grad_part + swap_band(activated_grad_part))[0]
    all_grads = gather_images(modulation_grad_half)
    all_activated = gather_images(activated)
    block_rows = features // lax.axis_size("img")
    own_activated = lax.dynamic_slice_in_dim(
        all_activated, lax.axis_index("img") * block_rows, block_rows, axis=1
    )
    modulation_grad_out = jnp.einsum(
        "id,ikc->dkc", own_activated, all_grads, preferred_element_type=jnp.float32
    )
    modulation_bias_out = jnp.sum(all_grads.astype(jnp.float32), axis=0)
    bias_parts = [
        query_bias_grad,
        value_bias_grad,
        project_bias_grad,
        expand_bias_grad,
        contract_bias_grad,
    ]
    bias_total = sum_all(jnp.concatenate(bias_parts))
    bias_outs = []
    place = 0
    for part in bias_parts:
        bias_outs.append(bias_total[place : place + part.shape[0]])
        place += part.shape[0]
    (
        query_bias_out,
        value_bias_out,
        project_bias_out,
        expand_bias_out,
        contract_bias_out,
    ) = bias_outs
    return (
        block_output,
        input_grad,
        conditioning_grad,
        modulation_grad_out,
        modulation_bias_out,
        attend_out,
        query_bias_out,
        value_bias_out,
        project_out,
        project_bias_out,
        expand_out,
        expand_bias_out,
        contract_out,
        contract_bias_out,
    )


def solution(mesh):
    in_specs = (
        P(("img", "band"), None),
        P("img", None),
        P(("img", "band")),
        P(("img", "band")),
        P(("img", "band")),
        P(None, "band", None),
        P("band", None),
        P(),
        P(),
        P(),
        P(),
        P(),
        P(),
        P(),
        P(),
        P(),
        P(("img", "band"), None),
    )
    out_specs = (
        P(("img", "band"), None),
        P(("img", "band"), None),
        P("img", None),
        P("img", "band", None),
        P("band", None),
        P("img", "band"),
        P(),
        P(),
        P("img", "band"),
        P(),
        P("img", "band"),
        P(),
        P("img", "band"),
        P(),
    )
    return jax.shard_map(shards, mesh=mesh, in_specs=in_specs, out_specs=out_specs, check_vma=False)
```

```python
import functools
import math

import jax
import jax.numpy as jnp
from jax import lax
from jax.experimental import pallas as pl
from jax.sharding import PartitionSpec as P

HEADS = 16


def layer_norm(values):
    row_mean = jnp.mean(values, axis=-1, keepdims=True)
    centred = values - row_mean
    spread = jnp.mean(centred * centred, axis=-1, keepdims=True)
    return centred * lax.rsqrt(spread + 1e-06)


def gelu_tanh(values):
    return (
        0.5
        * values
        * (1.0 + jnp.tanh(0.7978845608028654 * (values + 0.044715 * values * values * values)))
    )


def swish_gate(values):
    return values / (1.0 + jnp.exp(-values))


ROW_PLACES, COL_PLACES = 32, 64


def position_pieces(features):
    quarter = features // 4
    frequency = jnp.exp(-math.log(10000.0) * jnp.arange(quarter, dtype=jnp.float32) / quarter)
    angle = jnp.arange(COL_PLACES, dtype=jnp.float32)[:, None] * frequency[None, :]
    waves = jnp.concatenate([jnp.sin(angle), jnp.cos(angle)], axis=1)
    pieces = []
    for _ in range(3):
        piece = lax.reduce_precision(waves, 8, 7)
        pieces.append(piece.astype(jnp.bfloat16))
        waves = waves - piece
    blank = jnp.zeros_like(pieces[0])
    return jnp.concatenate(
        [jnp.concatenate([piece, blank], axis=1) for piece in pieces]
        + [jnp.concatenate([blank, piece], axis=1)[:ROW_PLACES] for piece in pieces],
        axis=0,
    )


def position_table(rows_in, cols_in, pieces):
    spot = jnp.arange(pieces.shape[0])[None, :]
    col_spots = 3 * COL_PLACES
    chosen = jnp.where(
        spot < col_spots,
        spot % COL_PLACES == cols_in[:, None],
        (spot - col_spots) % ROW_PLACES == rows_in[:, None],
    )
    return jnp.dot(chosen.astype(jnp.bfloat16), pieces, preferred_element_type=jnp.float32)


def norm_modulate(values, shift_rows, scale_rows):
    return layer_norm(values) * (1.0 + scale_rows[:, None, :]) + shift_rows[:, None, :]


def swap_bit(value, bit):
    members = lax.axis_size("img")
    return lax.ppermute(value, "img", [(i, i ^ (1 << bit)) for i in range(members)])


def swap_band(value):
    return lax.ppermute(value, "band", [(0, 1), (1, 0)])


def swap(value, stage):
    return swap_band(value) if stage == "band" else swap_bit(value, stage)


def my_bit(stage):
    if stage == "band":
        return lax.axis_index("band")
    return (lax.axis_index("img") >> stage) & 1


def pick(choice, if_zero, if_one):
    return jnp.where(choice == 0, if_zero, if_one)


def image_bits():
    return lax.axis_size("img").bit_length() - 1


def attend_kernel(score_scale, q_ref, k_ref, v_ref, kx_ref, vx_ref, mask_ref, out_ref, log_ref):
    keys = jnp.concatenate([k_ref[0], kx_ref[0]], axis=1)
    values = jnp.concatenate([v_ref[0], vx_ref[0]], axis=1)
    scores = lax.dot_general(
        keys, q_ref[0], (((0,), (0,)), ((), ())), preferred_element_type=jnp.float32
    )
    scores = jnp.where(mask_ref[...] > 0, scores * score_scale, -1e30)
    top = jnp.max(scores, axis=0, keepdims=True)
    weights = jnp.exp(scores - top)
    total = jnp.sum(weights, axis=0, keepdims=True)
    probabilities = (weights * (1.0 / total)).astype(jnp.bfloat16)
    out_ref[0] = jnp.dot(values, probabilities, preferred_element_type=jnp.float32).astype(
        jnp.bfloat16
    )
    log_ref[0] = top + jnp.log(total)


def head_blocks(size, rows, heads):
    block = lambda base: pl.BlockSpec((1, size, rows), lambda h: (base * heads + h, 0, 0))
    return [block(0), block(1), block(2), block(0), block(1)]


def attend_forward(own, other, mask, score_scale):
    heads, (_, size, rows) = HEADS, own.shape
    columns = 2 * rows
    return pl.pallas_call(
        functools.partial(attend_kernel, score_scale),
        grid=(heads,),
        in_specs=head_blocks(size, rows, heads)
        + [pl.BlockSpec((columns, 1), lambda h: (0, 0))],
        out_specs=[
            pl.BlockSpec((1, size, rows), lambda h: (h, 0, 0)),
            pl.BlockSpec((1, 1, rows), lambda h: (h, 0, 0)),
        ],
        out_shape=[
            jax.ShapeDtypeStruct((heads, size, rows), jnp.bfloat16),
            jax.ShapeDtypeStruct((heads, 1, rows), jnp.float32),
        ],
        cost_estimate=pl.CostEstimate(
            flops=16 * heads * 128 * rows * columns,
            bytes_accessed=4 * heads * size * (rows + columns),
            transcendentals=heads * rows * columns,
        ),
    )(own, own, own, other, other, mask)


def attend_back_kernel(
    score_scale,
    q_ref,
    k_ref,
    v_ref,
    kx_ref,
    vx_ref,
    go_ref,
    log_ref,
    mask_ref,
    dq_ref,
    own_ref,
    other_ref,
):
    queries, grads = q_ref[0], go_ref[0]
    keys = jnp.concatenate([k_ref[0], kx_ref[0]], axis=1)
    values = jnp.concatenate([v_ref[0], vx_ref[0]], axis=1)
    rows = queries.shape[1]

    def outer(left, right):
        return lax.dot_general(
            left, right, (((0,), (0,)), ((), ())), preferred_element_type=jnp.float32
        )

    def across(left, right):
        return lax.dot_general(
            left, right, (((1,), (1,)), ((), ())), preferred_element_type=jnp.float32
        )

    scores = jnp.where(mask_ref[...] > 0, outer(keys, queries) * score_scale, -1e30)
    weights = jnp.exp(scores - log_ref[0])
    grad_weights = outer(values, grads)
    delta = jnp.sum(weights * grad_weights, axis=0, keepdims=True)
    grad_scores = (weights * (grad_weights - delta)).astype(jnp.bfloat16)
    grad_values = across(grads, weights.astype(jnp.bfloat16))
    grad_keys = across(queries, grad_scores) * score_scale
    for i, grad in enumerate((grad_keys, grad_values)):
        own_ref[i, 0] = grad[:, :rows]
        other_ref[i, 0] = grad[:, rows:].astype(other_ref.dtype)
    dq_ref[0] = (
        jnp.dot(keys, grad_scores, preferred_element_type=jnp.float32) * score_scale
    ).astype(dq_ref.dtype)


def attend_backward(own, other, grads, log_total, mask, score_scale):
    heads, (_, size, rows) = HEADS, own.shape
    columns = 2 * rows
    single = pl.BlockSpec((1, size, rows), lambda h: (h, 0, 0))
    double = pl.BlockSpec((2, 1, size, rows), lambda h: (0, h, 0, 0))
    return pl.pallas_call(
        functools.partial(attend_back_kernel, score_scale),
        grid=(heads,),
        in_specs=head_blocks(size, rows, heads)
        + [
            single,
            pl.BlockSpec((1, 1, rows), lambda h: (h, 0, 0)),
            pl.BlockSpec((columns, 1), lambda h: (0, 0)),
        ],
        out_specs=[single, double, double],
        out_shape=[
            jax.ShapeDtypeStruct((heads, size, rows), jnp.bfloat16),
            jax.ShapeDtypeStruct((2, heads, size, rows), jnp.float32),
            jax.ShapeDtypeStruct((2, heads, size, rows), jnp.bfloat16),
        ],
        cost_estimate=pl.CostEstimate(
            flops=30 * heads * 128 * rows * columns,
            bytes_accessed=8 * heads * size * (rows + columns),
            transcendentals=heads * rows * columns,
        ),
    )(own, own, own, other, other, grads, log_total, mask)


def column_tile(width):
    return 384 if width % 384 == 0 else width


def project_kernel(rows_ref, weight_ref, bias_ref, out_ref):
    flat = jnp.dot(rows_ref[...], weight_ref[...], preferred_element_type=jnp.float32)
    out_ref[...] = (flat + bias_ref[...].astype(jnp.float32)).T.astype(out_ref.dtype)


def project_rows(rows, weight, bias, skip):
    depth = weight.shape[0]
    width = weight.shape[1] - skip
    tile = column_tile(depth)
    first = skip // tile
    return pl.pallas_call(
        project_kernel,
        grid=(width // tile,),
        in_specs=[
            pl.BlockSpec(rows.shape, lambda n: (0, 0)),
            pl.BlockSpec((depth, tile), lambda n: (0, n + first)),
            pl.BlockSpec((1, tile), lambda n: (0, n + first)),
        ],
        out_specs=pl.BlockSpec((tile, rows.shape[0]), lambda n: (n, 0)),
        out_shape=jax.ShapeDtypeStruct((width, rows.shape[0]), jnp.bfloat16),
        cost_estimate=pl.CostEstimate(
            flops=2 * rows.shape[0] * depth * width,
            bytes_accessed=2 * depth * width,
            transcendentals=0,
        ),
    )(rows, weight, bias)


def product_kernel(
    left_axis, right_axis, columns, orders, per_step, left_ref, left_far, right_ref,
    right_far, *out_refs
):
    contract = (((left_axis,), (right_axis,)), ((), ()))
    near = lax.dot_general(
        left_ref[...], right_ref[...], contract, preferred_element_type=jnp.float32
    )
    far = lax.dot_general(
        left_far[...], right_far[...], contract, preferred_element_type=jnp.float32
    )
    total = (near + far).astype(jnp.bfloat16)
    padded = total.shape[1] // 2
    chunk = total.shape[0] // per_step
    part = chunk // len(orders)

    def piece(band, index, i):
        start = index * chunk + i * part
        return total[start : start + part, band * padded : band * padded + columns]

    for i, order in enumerate(orders):
        going_ref, staying_ref = out_refs[2 * i], out_refs[2 * i + 1]
        if order[0] == "band":
            for index in range(per_step):
                going_ref[index] = piece(0, index, i)
                staying_ref[index] = piece(1, index, i)
        else:
            side = (lax.axis_index("img") >> order[0]) & 1
            step = 1 << (order[0] - 1)
            slot = 0
            for index in range(per_step):
                if index & step:
                    continue
                for band in range(2):
                    first, second = piece(band, index, i), piece(band, index | step, i)
                    going_ref[band, slot] = jnp.where(side == 0, second, first)
                    staying_ref[band, slot] = jnp.where(side == 0, first, second)
                slot += 1


def row_product(left, left_far, right, right_far, left_axis, right_axis, columns, orders):
    depth, width = left.shape[left_axis], left.shape[1 - left_axis]
    bits = image_bits()
    chunks = 1 << (bits - 1)
    tile = width // 4 if width > 2 * right.shape[1 - right_axis] else width
    per_step = chunks * tile // width
    part = width // chunks // len(orders)
    left_block = (
        pl.BlockSpec((depth, tile), lambda k: (0, k))
        if left_axis == 0
        else pl.BlockSpec((tile, depth), lambda k: (k, 0))
    )
    right_block = pl.BlockSpec(right.shape, lambda k: (0, 0))
    out_specs, out_shape = [], []
    for order in orders:
        if order[0] == "band":
            shape, block = (chunks, part, columns), (per_step, part, columns)
            spec = pl.BlockSpec(block, lambda k: (k, 0, 0))
        else:
            shape = (2, chunks // 2, part, columns)
            spec = pl.BlockSpec((2, per_step // 2, part, columns), lambda k: (0, k, 0, 0))
        out_specs += [spec, spec]
        out_shape += [jax.ShapeDtypeStruct(shape, jnp.bfloat16)] * 2
    outs = pl.pallas_call(
        functools.partial(
            product_kernel, left_axis, right_axis, columns, orders, per_step
        ),
        grid=(width // tile,),
        in_specs=[left_block, left_block, right_block, right_block],
        out_specs=out_specs,
        out_shape=out_shape,
        cost_estimate=pl.CostEstimate(
            flops=8 * depth * width * columns,
            bytes_accessed=8 * depth * (width + columns) + 4 * width * columns,
            transcendentals=0,
        ),
    )(left, left_far, right, right_far)
    halves = []
    for i, order in enumerate(orders):
        left_bits = ["band"] + list(range(bits - 1, 0, -1))
        left_bits.remove(order[0])
        shape = (2,) * len(left_bits) + (part, columns)
        halves.append((outs[2 * i].reshape(shape), outs[2 * i + 1].reshape(shape)))
    return halves


def core_columns(values, axis, core, band):
    quarter = values.shape[axis] // 4
    pieces = [lax.slice_in_dim(values, i * quarter, (i + 1) * quarter, axis=axis) for i in range(4)]
    return pick(
        band, pick(core, pieces[0], pieces[1]), pick(core, pieces[2], pieces[3])
    )


def chip_product(left, right, orders, left_axis=0, right_axis=0):
    core, band = my_bit(0), my_bit("band")
    axis = 1 - right_axis
    columns = right.shape[axis] // 4
    edges = [(0, 0), (0, 0)]
    edges[axis] = (0, -columns % 128)

    def chosen(which):
        return jnp.concatenate(
            [jnp.pad(core_columns(right, axis, which, b), edges) for b in (1 - band, band)],
            axis=axis,
        )

    left_far, right_far = swap_bit(left, 0), swap_bit(chosen(1 - core), 0)
    return row_product(
        left, left_far, chosen(core), right_far, left_axis, right_axis, columns, orders
    )


def scatter_sum(halves, orders):
    core = my_bit(0)
    totals = [scatter_part(*pair, order) for pair, order in zip(halves, orders)]
    total = jnp.concatenate(totals, axis=0) if len(totals) > 1 else totals[0]
    rows = total.shape[0] // 2
    low, high = total[:rows], total[rows:]
    here, there = pick(core, low, high), swap_bit(pick(core, high, low), 0)
    return pick(
        core,
        jnp.concatenate([here, there], axis=1),
        jnp.concatenate([there, here], axis=1),
    )


def scatter_part(going, staying, order):
    alive = ["band"] + list(range(image_bits() - 1, 0, -1))
    for stage in order:
        axis = alive.index(stage)
        alive.remove(stage)
        if stage != order[0]:
            first = lax.index_in_dim(block, 0, axis, keepdims=False)
            second = lax.index_in_dim(block, 1, axis, keepdims=False)
            if stage == "band":
                going, staying = first, second
            else:
                side = my_bit(stage)
                going, staying = pick(side, second, first), pick(side, first, second)
        block = staying.astype(jnp.float32) + swap(going, stage).astype(jnp.float32)
        if stage != order[-1]:
            block = block.astype(jnp.bfloat16)
    return block


def sum_all(value):
    for stage in ["band"] + list(range(image_bits())):
        value = value + swap(value, stage)
    return value


def gather_images(value):
    for stage in range(image_bits()):
        other = swap_bit(value, stage)
        side = my_bit(stage)
        value = jnp.concatenate([pick(side, value, other), pick(side, other, value)], axis=0)
    return value


def shards(
    block_input,
    conditioning,
    patch_valid,
    pos_rows,
    pos_cols,
    modulation_weight,
    modulation_bias,
    attend_weight,
    query_bias,
    value_bias,
    project_weight,
    project_bias,
    expand_weight,
    expand_bias,
    contract_weight,
    contract_bias,
    out_cotangent,
):
    slot_count, features = block_input.shape
    image_count = conditioning.shape[0]
    per_image = slot_count // image_count
    head_count = HEADS
    rest = list(range(2, image_bits()))
    y_first = ["band", 1] + rest
    x_first = [1] + rest + ["band"]
    z_first = rest + ["band", 1]
    head_size = features // head_count
    score_scale = 1.0 / math.sqrt(head_size)
    valid_rows = patch_valid.astype(jnp.float32)
    band = lax.axis_index("band")
    other_places = swap_band(jnp.stack([pos_rows, pos_cols, patch_valid]))
    sent_input, other_places = lax.optimization_barrier((block_input, other_places))
    other_input = swap_band(sent_input)
    pieces = position_pieces(features)
    pos_table = position_table(pos_rows, pos_cols, pieces)
    other_table = position_table(other_places[0], other_places[1], pieces)
    hidden = block_input.astype(jnp.float32) + pos_table
    shaped = hidden.reshape(image_count, per_image, features)
    cond_float = conditioning.astype(jnp.float32)
    swish_value, swish_back = jax.vjp(swish_gate, cond_float)
    activated = swish_value.astype(jnp.bfloat16)
    modulation_half = jnp.einsum(
        "id,dkc->ikc", activated, modulation_weight, preferred_element_type=jnp.float32
    ) + modulation_bias.astype(jnp.float32)
    modulation_other = swap_band(modulation_half)
    modulation = jnp.concatenate(
        [
            pick(band, modulation_half, modulation_other),
            pick(band, modulation_other, modulation_half),
        ],
        axis=1,
    )
    shift_one, scale_one, gate_one = (modulation[:, 0], modulation[:, 1], modulation[:, 2])
    shift_two, scale_two, gate_two = (modulation[:, 3], modulation[:, 4], modulation[:, 5])
    first_mod, first_back = jax.vjp(norm_modulate, shaped, shift_one, scale_one)
    first_low = first_mod.astype(jnp.bfloat16).reshape(slot_count, features)
    input_bias = jnp.concatenate([query_bias, jnp.zeros_like(query_bias), value_bias])[None, :]

    def project_heads(rows, skip):
        flat = project_rows(rows, attend_weight, input_bias, skip)
        return flat.reshape(-1, head_size, slot_count)

    own_heads = project_heads(first_low, 0)
    other_shaped = (other_input.astype(jnp.float32) + other_table).reshape(
        image_count, per_image, features
    )
    other_low = (
        norm_modulate(other_shaped, shift_one, scale_one)
        .astype(jnp.bfloat16)
        .reshape(slot_count, features)
    )
    other_heads = project_heads(other_low, features)
    key_mask = jnp.concatenate([patch_valid, other_places[2]]).astype(jnp.float32)[:, None]
    mixed_heads, log_total = attend_forward(own_heads, other_heads, key_mask, score_scale)
    mixed_low = mixed_heads.reshape(features, slot_count)
    branch = jnp.einsum(
        "et,ed->td", mixed_low, project_weight, preferred_element_type=jnp.float32
    ) + project_bias.astype(jnp.float32)
    branch_rows = branch.reshape(image_count, per_image, features)
    middle = shaped + gate_one[:, None, :] * branch_rows
    second_mod, second_back = jax.vjp(norm_modulate, middle, shift_two, scale_two)
    second_low = second_mod.astype(jnp.bfloat16).reshape(slot_count, features)
    expanded = jnp.dot(
        second_low, expand_weight, preferred_element_type=jnp.float32
    ) + expand_bias.astype(jnp.float32)
    activation, gelu_back = jax.vjp(gelu_tanh, expanded)
    activation_low = activation.astype(jnp.bfloat16)
    mlp_out = jnp.dot(
        activation_low, contract_weight, preferred_element_type=jnp.float32
    ) + contract_bias.astype(jnp.float32)
    mlp_rows = mlp_out.reshape(image_count, per_image, features)
    result = middle + gate_two[:, None, :] * mlp_rows
    block_output = result.reshape(slot_count, features).astype(jnp.bfloat16)
    upstream = (out_cotangent.astype(jnp.float32) * valid_rows[:, None]).reshape(
        image_count, per_image, features
    )
    grad_gate_two = jnp.sum(upstream * mlp_rows, axis=1)
    grad_mlp = (gate_two[:, None, :] * upstream).reshape(slot_count, features).astype(jnp.bfloat16)
    contract_chip = chip_product(activation_low, grad_mlp, [x_first])
    contract_bias_grad = jnp.sum(grad_mlp.astype(jnp.float32), axis=0)
    grad_activation = jnp.einsum(
        "td,fd->tf", grad_mlp, contract_weight, preferred_element_type=jnp.float32
    )
    grad_expanded = gelu_back(grad_activation)[0].astype(jnp.bfloat16)
    expand_chip = chip_product(second_low, grad_expanded, [y_first])
    expand_bias_grad = jnp.sum(grad_expanded.astype(jnp.float32), axis=0)
    grad_second = jnp.einsum(
        "tf,df->td", grad_expanded, expand_weight, preferred_element_type=jnp.float32
    )
    grad_norm_two, grad_shift_two, grad_scale_two = second_back(
        grad_second.reshape(image_count, per_image, features)
    )
    grad_middle = upstream + grad_norm_two
    grad_gate_one = jnp.sum(grad_middle * branch_rows, axis=1)
    grad_branch = (
        (gate_one[:, None, :] * grad_middle).reshape(slot_count, features).astype(jnp.bfloat16)
    )
    grad_branch, contract_chip, expand_chip = lax.optimization_barrier(
        (grad_branch, contract_chip, expand_chip)
    )
    contract_out = scatter_sum(contract_chip, [x_first])
    expand_out = scatter_sum(expand_chip, [y_first])
    project_out = scatter_sum(
        chip_product(mixed_low, grad_branch, [z_first], left_axis=1), [z_first]
    )
    project_bias_grad = jnp.sum(grad_branch.astype(jnp.float32), axis=0)
    grad_mixed = jnp.einsum(
        "td,ed->et", grad_branch, project_weight, preferred_element_type=jnp.float32
    ).astype(jnp.bfloat16)
    grad_query, grad_pair, grad_pair_other = attend_backward(
        own_heads,
        other_heads,
        grad_mixed.reshape(head_count, head_size, slot_count),
        log_total,
        key_mask,
        score_scale,
    )
    grad_pair = grad_pair + swap_band(grad_pair_other).astype(jnp.float32)
    grad_qkv = jnp.concatenate(
        [
            grad_query.reshape(features, slot_count),
            grad_pair.astype(jnp.bfloat16).reshape(2 * features, slot_count),
        ],
        axis=0,
    )
    thirds = [x_first, y_first, z_first]
    attend_out = scatter_sum(
        chip_product(first_low, grad_qkv, thirds, right_axis=1), thirds
    )
    query_bias_grad = jnp.sum(grad_qkv[:features].astype(jnp.float32), axis=1)
    value_bias_grad = jnp.sum(grad_qkv[2 * features :].astype(jnp.float32), axis=1)
    grad_first = jnp.einsum(
        "et,de->td", grad_qkv, attend_weight, preferred_element_type=jnp.float32
    )
    grad_norm_one, grad_shift_one, grad_scale_one = first_back(
        grad_first.reshape(image_count, per_image, features)
    )
    input_grad = (grad_middle + grad_norm_one).reshape(slot_count, features)
    grad_modulation = jnp.stack(
        [
            grad_shift_one,
            grad_scale_one,
            grad_gate_one,
            grad_shift_two,
            grad_scale_two,
            grad_gate_two,
        ],
        axis=1,
    )
    grad_halves = grad_modulation.reshape(image_count, 2, -1, features)
    modulation_grad_half = (
        pick(band, grad_halves[:, 0], grad_halves[:, 1])
        + swap_band(pick(band, grad_halves[:, 1], grad_halves[:, 0]))
    ).astype(jnp.bfloat16)
    activated_grad_part = jnp.einsum(
        "ikc,dkc->id", modulation_grad_half, modulation_weight, preferred_element_type=jnp.float32
    )
    conditioning_grad = swish_back(activated_grad_part + swap_band(activated_grad_part))[0]
    all_grads = gather_images(modulation_grad_half)
    all_activated = gather_images(activated)
    block_rows = features // lax.axis_size("img")
    own_activated = lax.dynamic_slice_in_dim(
        all_activated, lax.axis_index("img") * block_rows, block_rows, axis=1
    )
    modulation_grad_out = jnp.einsum(
        "id,ikc->dkc", own_activated, all_grads, preferred_element_type=jnp.float32
    )
    modulation_bias_out = jnp.sum(all_grads.astype(jnp.float32), axis=0)
    bias_parts = [
        query_bias_grad,
        value_bias_grad,
        project_bias_grad,
        expand_bias_grad,
        contract_bias_grad,
    ]
    bias_total = sum_all(jnp.concatenate(bias_parts))
    bias_outs = []
    place = 0
    for part in bias_parts:
        bias_outs.append(bias_total[place : place + part.shape[0]])
        place += part.shape[0]
    (
        query_bias_out,
        value_bias_out,
        project_bias_out,
        expand_bias_out,
        contract_bias_out,
    ) = bias_outs
    return (
        block_output,
        input_grad,
        conditioning_grad,
        modulation_grad_out,
        modulation_bias_out,
        attend_out,
        query_bias_out,
        value_bias_out,
        project_out,
        project_bias_out,
        expand_out,
        expand_bias_out,
        contract_out,
        contract_bias_out,
    )


def solution(mesh):
    in_specs = (
        P(("img", "band"), None),
        P("img", None),
        P(("img", "band")),
        P(("img", "band")),
        P(("img", "band")),
        P(None, "band", None),
        P("band", None),
        P(),
        P(),
        P(),
        P(),
        P(),
        P(),
        P(),
        P(),
        P(),
        P(("img", "band"), None),
    )
    out_specs = (
        P(("img", "band"), None),
        P(("img", "band"), None),
        P("img", None),
        P("img", "band", None),
        P("band", None),
        P("img", "band"),
        P(),
        P(),
        P("img", "band"),
        P(),
        P("img", "band"),
        P(),
        P("img", "band"),
        P(),
    )
    return jax.shard_map(shards, mesh=mesh, in_specs=in_specs, out_specs=out_specs, check_vma=False)
```

```python
import functools
import math

import jax
import jax.numpy as jnp
from jax import lax
from jax.experimental import pallas as pl
from jax.sharding import PartitionSpec as P


HEADS = 16


def layer_norm(values):
    row_mean = jnp.mean(values, axis=-1, keepdims=True)
    centred = values - row_mean
    spread = jnp.mean(centred * centred, axis=-1, keepdims=True)
    return centred * lax.rsqrt(spread + 1e-06)


def gelu_tanh(values):
    return (
        0.5
        * values
        * (1.0 + jnp.tanh(0.7978845608028654 * (values + 0.044715 * values * values * values)))
    )


def swish_gate(values):
    return values / (1.0 + jnp.exp(-values))


ROW_PLACES, COL_PLACES = 32, 64


def position_pieces(features):
    quarter = features // 4
    frequency = jnp.exp(-math.log(10000.0) * jnp.arange(quarter, dtype=jnp.float32) / quarter)
    angle = jnp.arange(COL_PLACES, dtype=jnp.float32)[:, None] * frequency[None, :]
    waves = jnp.concatenate([jnp.sin(angle), jnp.cos(angle)], axis=1)
    pieces = []
    for _ in range(3):
        piece = lax.reduce_precision(waves, 8, 7)
        pieces.append(piece.astype(jnp.bfloat16))
        waves = waves - piece
    blank = jnp.zeros_like(pieces[0])
    return jnp.concatenate(
        [jnp.concatenate([piece, blank], axis=1) for piece in pieces]
        + [jnp.concatenate([blank, piece], axis=1)[:ROW_PLACES] for piece in pieces],
        axis=0,
    )


def position_table(rows_in, cols_in, pieces):
    spot = jnp.arange(pieces.shape[0])[None, :]
    col_spots = 3 * COL_PLACES
    chosen = jnp.where(
        spot < col_spots,
        spot % COL_PLACES == cols_in[:, None],
        (spot - col_spots) % ROW_PLACES == rows_in[:, None],
    )
    return jnp.dot(chosen.astype(jnp.bfloat16), pieces, preferred_element_type=jnp.float32)


def norm_modulate(values, shift_rows, scale_rows):
    return layer_norm(values) * (1.0 + scale_rows[:, None, :]) + shift_rows[:, None, :]


def swap_bit(value, bit):
    members = lax.axis_size("img")
    return lax.ppermute(value, "img", [(i, i ^ (1 << bit)) for i in range(members)])


def swap_band(value):
    return lax.ppermute(value, "band", [(0, 1), (1, 0)])


def swap(value, stage):
    return swap_band(value) if stage == "band" else swap_bit(value, stage)


def my_bit(stage):
    if stage == "band":
        return lax.axis_index("band")
    return (lax.axis_index("img") >> stage) & 1


def pick(choice, if_zero, if_one):
    return jnp.where(choice == 0, if_zero, if_one)


def image_bits():
    return lax.axis_size("img").bit_length() - 1


def attend_kernel(score_scale, q_ref, k_ref, v_ref, kx_ref, vx_ref, mask_ref, out_ref, log_ref):
    keys = jnp.concatenate([k_ref[0], kx_ref[0]], axis=1)
    values = jnp.concatenate([v_ref[0], vx_ref[0]], axis=1)
    scores = lax.dot_general(
        keys, q_ref[0], (((0,), (0,)), ((), ())), preferred_element_type=jnp.float32
    )
    scores = jnp.where(mask_ref[...] > 0, scores * score_scale, -1e30)
    top = jnp.max(scores, axis=0, keepdims=True)
    weights = jnp.exp(scores - top)
    total = jnp.sum(weights, axis=0, keepdims=True)
    probabilities = (weights * (1.0 / total)).astype(jnp.bfloat16)
    out_ref[0] = jnp.dot(values, probabilities, preferred_element_type=jnp.float32).astype(
        jnp.bfloat16
    )
    log_ref[0] = top + jnp.log(total)


def head_blocks(size, rows, heads):
    block = lambda base: pl.BlockSpec((1, size, rows), lambda h: (base * heads + h, 0, 0))
    return [block(0), block(1), block(2), block(0), block(1)]


def attend_forward(own, other, mask, score_scale):
    heads, (_, size, rows) = HEADS, own.shape
    columns = 2 * rows
    return pl.pallas_call(
        functools.partial(attend_kernel, score_scale),
        grid=(heads,),
        in_specs=head_blocks(size, rows, heads)
        + [pl.BlockSpec((columns, 1), lambda h: (0, 0))],
        out_specs=[
            pl.BlockSpec((1, size, rows), lambda h: (h, 0, 0)),
            pl.BlockSpec((1, 1, rows), lambda h: (h, 0, 0)),
        ],
        out_shape=[
            jax.ShapeDtypeStruct((heads, size, rows), jnp.bfloat16),
            jax.ShapeDtypeStruct((heads, 1, rows), jnp.float32),
        ],
        cost_estimate=pl.CostEstimate(
            flops=16 * heads * 128 * rows * columns,
            bytes_accessed=4 * heads * size * (rows + columns),
            transcendentals=heads * rows * columns,
        ),
    )(own, own, own, other, other, mask)


def attend_back_kernel(
    score_scale,
    q_ref,
    k_ref,
    v_ref,
    kx_ref,
    vx_ref,
    go_ref,
    log_ref,
    mask_ref,
    dq_ref,
    own_ref,
    other_ref,
):
    queries, grads = q_ref[0], go_ref[0]
    keys = jnp.concatenate([k_ref[0], kx_ref[0]], axis=1)
    values = jnp.concatenate([v_ref[0], vx_ref[0]], axis=1)
    rows = queries.shape[1]

    def outer(left, right):
        return lax.dot_general(
            left, right, (((0,), (0,)), ((), ())), preferred_element_type=jnp.float32
        )

    def across(left, right):
        return lax.dot_general(
            left, right, (((1,), (1,)), ((), ())), preferred_element_type=jnp.float32
        )

    scores = jnp.where(mask_ref[...] > 0, outer(keys, queries) * score_scale, -1e30)
    weights = jnp.exp(scores - log_ref[0])
    grad_weights = outer(values, grads)
    delta = jnp.sum(weights * grad_weights, axis=0, keepdims=True)
    grad_scores = (weights * (grad_weights - delta)).astype(jnp.bfloat16)
    grad_values = across(grads, weights.astype(jnp.bfloat16))
    grad_keys = across(queries, grad_scores) * score_scale
    for i, grad in enumerate((grad_keys, grad_values)):
        own_ref[i, 0] = grad[:, :rows]
        other_ref[i, 0] = grad[:, rows:].astype(other_ref.dtype)
    dq_ref[0] = (
        jnp.dot(keys, grad_scores, preferred_element_type=jnp.float32) * score_scale
    ).astype(dq_ref.dtype)


def attend_backward(own, other, grads, log_total, mask, score_scale):
    heads, (_, size, rows) = HEADS, own.shape
    columns = 2 * rows
    single = pl.BlockSpec((1, size, rows), lambda h: (h, 0, 0))
    double = pl.BlockSpec((2, 1, size, rows), lambda h: (0, h, 0, 0))
    return pl.pallas_call(
        functools.partial(attend_back_kernel, score_scale),
        grid=(heads,),
        in_specs=head_blocks(size, rows, heads)
        + [
            single,
            pl.BlockSpec((1, 1, rows), lambda h: (h, 0, 0)),
            pl.BlockSpec((columns, 1), lambda h: (0, 0)),
        ],
        out_specs=[single, double, double],
        out_shape=[
            jax.ShapeDtypeStruct((heads, size, rows), jnp.bfloat16),
            jax.ShapeDtypeStruct((2, heads, size, rows), jnp.float32),
            jax.ShapeDtypeStruct((2, heads, size, rows), jnp.bfloat16),
        ],
        cost_estimate=pl.CostEstimate(
            flops=30 * heads * 128 * rows * columns,
            bytes_accessed=8 * heads * size * (rows + columns),
            transcendentals=heads * rows * columns,
        ),
    )(own, own, own, other, other, grads, log_total, mask)


def column_tile(width):
    return 384 if width % 384 == 0 else width


def project_kernel(rows_ref, weight_ref, bias_ref, out_ref):
    flat = jnp.dot(rows_ref[...], weight_ref[...], preferred_element_type=jnp.float32)
    out_ref[...] = (flat + bias_ref[...].astype(jnp.float32)).T.astype(out_ref.dtype)


def project_rows(rows, weight, bias, skip):
    depth = weight.shape[0]
    width = weight.shape[1] - skip
    tile = column_tile(depth)
    first = skip // tile
    return pl.pallas_call(
        project_kernel,
        grid=(width // tile,),
        in_specs=[
            pl.BlockSpec(rows.shape, lambda n: (0, 0)),
            pl.BlockSpec((depth, tile), lambda n: (0, n + first)),
            pl.BlockSpec((1, tile), lambda n: (0, n + first)),
        ],
        out_specs=pl.BlockSpec((tile, rows.shape[0]), lambda n: (n, 0)),
        out_shape=jax.ShapeDtypeStruct((width, rows.shape[0]), jnp.bfloat16),
        cost_estimate=pl.CostEstimate(
            flops=2 * rows.shape[0] * depth * width,
            bytes_accessed=2 * depth * width,
            transcendentals=0,
        ),
    )(rows, weight, bias)


def product_kernel(
    left_axis, right_axis, columns, orders, per_step, left_ref, left_far, right_ref,
    right_far, *out_refs
):
    contract = (((left_axis,), (right_axis,)), ((), ()))
    near = lax.dot_general(
        left_ref[...], right_ref[...], contract, preferred_element_type=jnp.float32
    )
    far = lax.dot_general(
        left_far[...], right_far[...], contract, preferred_element_type=jnp.float32
    )
    total = (near + far).astype(jnp.bfloat16)
    padded = total.shape[1] // 2
    chunk = total.shape[0] // per_step
    part = chunk // len(orders)

    def piece(band, index, i):
        start = index * chunk + i * part
        return total[start : start + part, band * padded : band * padded + columns]

    for i, order in enumerate(orders):
        going_ref, staying_ref = out_refs[2 * i], out_refs[2 * i + 1]
        if order[0] == "band":
            for index in range(per_step):
                going_ref[index] = piece(0, index, i)
                staying_ref[index] = piece(1, index, i)
        else:
            side = (lax.axis_index("img") >> order[0]) & 1
            step = 1 << (order[0] - 1)
            slot = 0
            for index in range(per_step):
                if index & step:
                    continue
                for band in range(2):
                    first, second = piece(band, index, i), piece(band, index | step, i)
                    going_ref[band, slot] = jnp.where(side == 0, second, first)
                    staying_ref[band, slot] = jnp.where(side == 0, first, second)
                slot += 1


def row_product(left, left_far, right, right_far, left_axis, right_axis, columns, orders):
    depth, width = left.shape[left_axis], left.shape[1 - left_axis]
    bits = image_bits()
    chunks = 1 << (bits - 1)
    tile = width // 4 if width > 2 * right.shape[1 - right_axis] else width
    per_step = chunks * tile // width
    part = width // chunks // len(orders)
    left_block = (
        pl.BlockSpec((depth, tile), lambda k: (0, k))
        if left_axis == 0
        else pl.BlockSpec((tile, depth), lambda k: (k, 0))
    )
    right_block = pl.BlockSpec(right.shape, lambda k: (0, 0))
    out_specs, out_shape = [], []
    for order in orders:
        if order[0] == "band":
            shape, block = (chunks, part, columns), (per_step, part, columns)
            spec = pl.BlockSpec(block, lambda k: (k, 0, 0))
        else:
            shape = (2, chunks // 2, part, columns)
            spec = pl.BlockSpec((2, per_step // 2, part, columns), lambda k: (0, k, 0, 0))
        out_specs += [spec, spec]
        out_shape += [jax.ShapeDtypeStruct(shape, jnp.bfloat16)] * 2
    outs = pl.pallas_call(
        functools.partial(
            product_kernel, left_axis, right_axis, columns, orders, per_step
        ),
        grid=(width // tile,),
        in_specs=[left_block, left_block, right_block, right_block],
        out_specs=out_specs,
        out_shape=out_shape,
        cost_estimate=pl.CostEstimate(
            flops=8 * depth * width * columns,
            bytes_accessed=8 * depth * (width + columns) + 4 * width * columns,
            transcendentals=0,
        ),
    )(left, left_far, right, right_far)
    halves = []
    for i, order in enumerate(orders):
        left_bits = ["band"] + list(range(bits - 1, 0, -1))
        left_bits.remove(order[0])
        shape = (2,) * len(left_bits) + (part, columns)
        halves.append((outs[2 * i].reshape(shape), outs[2 * i + 1].reshape(shape)))
    return halves


def core_columns(values, axis, core, band):
    quarter = values.shape[axis] // 4
    pieces = [lax.slice_in_dim(values, i * quarter, (i + 1) * quarter, axis=axis) for i in range(4)]
    return pick(
        band, pick(core, pieces[0], pieces[1]), pick(core, pieces[2], pieces[3])
    )


def halved_kernel(columns, part, left_ref, left_far, right_ref, right_far, going_ref, staying_ref):
    core = lax.axis_index("img") & 1
    chips = left_ref.shape[1] // (2 * part)

    def own_rows(ref):
        rows = ref[...].T
        pieces = [rows[i * part : (i + 1) * part] for i in range(2 * chips)]
        return jnp.concatenate(
            [jnp.where(core == 0, pieces[2 * i], pieces[2 * i + 1]) for i in range(chips)], axis=0
        )

    near = jnp.dot(own_rows(left_ref), right_ref[...], preferred_element_type=jnp.float32)
    far = jnp.dot(own_rows(left_far), right_far[...], preferred_element_type=jnp.float32)
    total = (near + far).astype(jnp.bfloat16)
    padded = total.shape[1] // 2
    side = (lax.axis_index("img") >> 1) & 1
    for i in range(2):
        pieces = [
            total[x * part : (x + 1) * part, i * padded : i * padded + columns]
            for x in range(chips)
        ]
        for x in range(chips // 2):
            first, second = pieces[2 * x], pieces[2 * x + 1]
            going_ref[i, x] = jnp.where(side == 0, second, first)
            staying_ref[i, x] = jnp.where(side == 0, first, second)


def halved_product(left, right):
    depth, width = left.shape
    bits = image_bits()
    chips = 1 << (bits - 1)
    band = my_bit("band")
    columns = right.shape[1] // 2
    halves = [right[:, :columns], right[:, columns:]]
    right = jnp.concatenate(
        [
            jnp.pad(pick(band, *pair), [(0, 0), (0, -columns % 128)])
            for pair in (halves[::-1], halves)
        ],
        axis=1,
    )
    right_far = swap_bit(right, 0)
    tile, part = width // 4, width // chips // 2
    left_block = pl.BlockSpec((depth, tile), lambda k: (0, k))
    right_block = pl.BlockSpec(right.shape, lambda k: (0, 0))
    out_block = pl.BlockSpec((2, chips // 8, part, columns), lambda k: (0, k, 0, 0))
    out_shape = jax.ShapeDtypeStruct((2, chips // 2, part, columns), jnp.bfloat16)
    going, staying = pl.pallas_call(
        functools.partial(halved_kernel, columns, part),
        grid=(4,),
        in_specs=[left_block, left_block, right_block, right_block],
        out_specs=[out_block, out_block],
        out_shape=[out_shape, out_shape],
        cost_estimate=pl.CostEstimate(
            flops=4 * depth * width * columns,
            bytes_accessed=8 * depth * (width + columns) + 4 * width * columns,
            transcendentals=0,
        ),
    )(left, swap_bit(left, 0), right, right_far)
    shape = (2,) * (bits - 1) + (part, columns)
    return going.reshape(shape), staying.reshape(shape)


def chip_product(left, right, orders, left_axis=0, right_axis=0):
    core, band = my_bit(0), my_bit("band")
    axis = 1 - right_axis
    columns = right.shape[axis] // 4
    edges = [(0, 0), (0, 0)]
    edges[axis] = (0, -columns % 128)

    def chosen(which):
        return jnp.concatenate(
            [jnp.pad(core_columns(right, axis, which, b), edges) for b in (1 - band, band)],
            axis=axis,
        )

    left_far, right_far = swap_bit(left, 0), swap_bit(chosen(1 - core), 0)
    return row_product(
        left, left_far, chosen(core), right_far, left_axis, right_axis, columns, orders
    )


def scatter_sum(halves, orders):
    core = my_bit(0)
    totals = [scatter_part(*pair, order) for pair, order in zip(halves, orders)]
    total = jnp.concatenate(totals, axis=0) if len(totals) > 1 else totals[0]
    rows = total.shape[0] // 2
    low, high = total[:rows], total[rows:]
    here, there = pick(core, low, high), swap_bit(pick(core, high, low), 0)
    return pick(
        core,
        jnp.concatenate([here, there], axis=1),
        jnp.concatenate([there, here], axis=1),
    )


def scatter_part(going, staying, order):
    alive = ["band"] + list(range(image_bits() - 1, 0, -1))
    for stage in order:
        axis = alive.index(stage)
        alive.remove(stage)
        if stage != order[0]:
            first = lax.index_in_dim(block, 0, axis, keepdims=False)
            second = lax.index_in_dim(block, 1, axis, keepdims=False)
            if stage == "band":
                going, staying = first, second
            else:
                side = my_bit(stage)
                going, staying = pick(side, second, first), pick(side, first, second)
        arrived = swap(going, stage)
        block = staying.astype(jnp.float32) + arrived.astype(jnp.float32)
        if stage != order[-1]:
            block = block.astype(jnp.bfloat16)
    return block


def sum_all(value):
    for stage in ["band"] + list(range(image_bits())):
        value = value + swap(value, stage)
    return value


def gather_images(value):
    for stage in range(image_bits()):
        other = swap_bit(value, stage)
        side = my_bit(stage)
        value = jnp.concatenate([pick(side, value, other), pick(side, other, value)], axis=0)
    return value


def shards(
    block_input,
    conditioning,
    patch_valid,
    pos_rows,
    pos_cols,
    modulation_weight,
    modulation_bias,
    attend_weight,
    query_bias,
    value_bias,
    project_weight,
    project_bias,
    expand_weight,
    expand_bias,
    contract_weight,
    contract_bias,
    out_cotangent,
):
    slot_count, features = block_input.shape
    image_count = conditioning.shape[0]
    per_image = slot_count // image_count
    head_count = HEADS
    rest = list(range(3, image_bits()))
    expand_order = [2, 1, "band"] + rest
    contract_order = [1, 2, "band"] + rest
    project_order = ["band", 2, 1] + rest
    attend_orders = [[1, "band", 2] + rest, ["band", 2, 1] + rest, [2, 1, "band"] + rest]
    head_size = features // head_count
    score_scale = 1.0 / math.sqrt(head_size)
    valid_rows = patch_valid.astype(jnp.float32)
    band = lax.axis_index("band")
    other_places = swap_band(jnp.stack([pos_rows, pos_cols, patch_valid]))
    sent_input, other_places = lax.optimization_barrier((block_input, other_places))
    other_input = swap_band(sent_input)
    pieces = position_pieces(features)
    pos_table = position_table(pos_rows, pos_cols, pieces)
    other_table = position_table(other_places[0], other_places[1], pieces)
    hidden = block_input.astype(jnp.float32) + pos_table
    shaped = hidden.reshape(image_count, per_image, features)
    cond_float = conditioning.astype(jnp.float32)
    swish_value, swish_back = jax.vjp(swish_gate, cond_float)
    activated = swish_value.astype(jnp.bfloat16)
    modulation_half = jnp.einsum(
        "id,dkc->ikc", activated, modulation_weight, preferred_element_type=jnp.float32
    ) + modulation_bias.astype(jnp.float32)
    modulation_other = swap_band(modulation_half)
    modulation = jnp.concatenate(
        [
            pick(band, modulation_half, modulation_other),
            pick(band, modulation_other, modulation_half),
        ],
        axis=1,
    )
    shift_one, scale_one, gate_one = (modulation[:, 0], modulation[:, 1], modulation[:, 2])
    shift_two, scale_two, gate_two = (modulation[:, 3], modulation[:, 4], modulation[:, 5])
    first_mod, first_back = jax.vjp(norm_modulate, shaped, shift_one, scale_one)
    first_low = first_mod.astype(jnp.bfloat16).reshape(slot_count, features)
    input_bias = jnp.concatenate([query_bias, jnp.zeros_like(query_bias), value_bias])[None, :]

    def project_heads(rows, skip):
        flat = project_rows(rows, attend_weight, input_bias, skip)
        return flat.reshape(-1, head_size, slot_count)

    own_heads = project_heads(first_low, 0)
    other_shaped = (other_input.astype(jnp.float32) + other_table).reshape(
        image_count, per_image, features
    )
    other_low = (
        norm_modulate(other_shaped, shift_one, scale_one)
        .astype(jnp.bfloat16)
        .reshape(slot_count, features)
    )
    other_heads = project_heads(other_low, features)
    key_mask = jnp.concatenate([patch_valid, other_places[2]]).astype(jnp.float32)[:, None]
    mixed_heads, log_total = attend_forward(own_heads, other_heads, key_mask, score_scale)
    mixed_low = mixed_heads.reshape(features, slot_count)
    branch = jnp.einsum(
        "et,ed->td", mixed_low, project_weight, preferred_element_type=jnp.float32
    ) + project_bias.astype(jnp.float32)
    branch_rows = branch.reshape(image_count, per_image, features)
    middle = shaped + gate_one[:, None, :] * branch_rows
    second_mod, second_back = jax.vjp(norm_modulate, middle, shift_two, scale_two)
    second_low = second_mod.astype(jnp.bfloat16).reshape(slot_count, features)
    expanded = jnp.dot(
        second_low, expand_weight, preferred_element_type=jnp.float32
    ) + expand_bias.astype(jnp.float32)
    activation, gelu_back = jax.vjp(gelu_tanh, expanded)
    activation_low = activation.astype(jnp.bfloat16)
    mlp_out = jnp.dot(
        activation_low, contract_weight, preferred_element_type=jnp.float32
    ) + contract_bias.astype(jnp.float32)
    mlp_rows = mlp_out.reshape(image_count, per_image, features)
    result = middle + gate_two[:, None, :] * mlp_rows
    block_output = result.reshape(slot_count, features).astype(jnp.bfloat16)
    upstream = (out_cotangent.astype(jnp.float32) * valid_rows[:, None]).reshape(
        image_count, per_image, features
    )
    grad_gate_two = jnp.sum(upstream * mlp_rows, axis=1)
    grad_mlp = (gate_two[:, None, :] * upstream).reshape(slot_count, features).astype(jnp.bfloat16)
    contract_chip = halved_product(activation_low, grad_mlp)
    contract_bias_grad = jnp.sum(grad_mlp.astype(jnp.float32), axis=0)
    grad_activation = jnp.einsum(
        "td,fd->tf", grad_mlp, contract_weight, preferred_element_type=jnp.float32
    )
    grad_expanded = gelu_back(grad_activation)[0].astype(jnp.bfloat16)
    expand_chip = chip_product(second_low, grad_expanded, [expand_order])
    expand_bias_grad = jnp.sum(grad_expanded.astype(jnp.float32), axis=0)
    grad_second = jnp.einsum(
        "tf,df->td", grad_expanded, expand_weight, preferred_element_type=jnp.float32
    )
    grad_norm_two, grad_shift_two, grad_scale_two = second_back(
        grad_second.reshape(image_count, per_image, features)
    )
    grad_middle = upstream + grad_norm_two
    grad_gate_one = jnp.sum(grad_middle * branch_rows, axis=1)
    grad_branch = (
        (gate_one[:, None, :] * grad_middle).reshape(slot_count, features).astype(jnp.bfloat16)
    )
    grad_branch, contract_chip, expand_chip = lax.optimization_barrier(
        (grad_branch, contract_chip, expand_chip)
    )
    contract_out = scatter_part(*contract_chip, contract_order)
    expand_out = scatter_sum(expand_chip, [expand_order])
    project_chip = chip_product(mixed_low, grad_branch, [project_order], left_axis=1)
    project_out = scatter_sum(project_chip, [project_order])
    project_bias_grad = jnp.sum(grad_branch.astype(jnp.float32), axis=0)
    grad_mixed = jnp.einsum(
        "td,ed->et", grad_branch, project_weight, preferred_element_type=jnp.float32
    ).astype(jnp.bfloat16)
    grad_query, grad_pair, grad_pair_other = attend_backward(
        own_heads,
        other_heads,
        grad_mixed.reshape(head_count, head_size, slot_count),
        log_total,
        key_mask,
        score_scale,
    )
    grad_pair_far = swap_band(grad_pair_other)
    grad_pair = grad_pair + grad_pair_far.astype(jnp.float32)
    grad_qkv = jnp.concatenate(
        [
            grad_query.reshape(features, slot_count),
            grad_pair.astype(jnp.bfloat16).reshape(2 * features, slot_count),
        ],
        axis=0,
    )
    attend_chip = chip_product(first_low, grad_qkv, attend_orders, right_axis=1)
    attend_out = scatter_sum(attend_chip, attend_orders)
    query_bias_grad = jnp.sum(grad_qkv[:features].astype(jnp.float32), axis=1)
    value_bias_grad = jnp.sum(grad_qkv[2 * features :].astype(jnp.float32), axis=1)
    grad_first = jnp.einsum(
        "et,de->td", grad_qkv, attend_weight, preferred_element_type=jnp.float32
    )
    grad_norm_one, grad_shift_one, grad_scale_one = first_back(
        grad_first.reshape(image_count, per_image, features)
    )
    input_grad = (grad_middle + grad_norm_one).reshape(slot_count, features)
    grad_modulation = jnp.stack(
        [
            grad_shift_one,
            grad_scale_one,
            grad_gate_one,
            grad_shift_two,
            grad_scale_two,
            grad_gate_two,
        ],
        axis=1,
    )
    grad_halves = grad_modulation.reshape(image_count, 2, -1, features)
    modulation_grad_half = (
        pick(band, grad_halves[:, 0], grad_halves[:, 1])
        + swap_band(pick(band, grad_halves[:, 1], grad_halves[:, 0]))
    ).astype(jnp.bfloat16)
    activated_grad_part = jnp.einsum(
        "ikc,dkc->id", modulation_grad_half, modulation_weight, preferred_element_type=jnp.float32
    )
    conditioning_grad = swish_back(activated_grad_part + swap_band(activated_grad_part))[0]
    all_grads = gather_images(modulation_grad_half)
    all_activated = gather_images(activated)
    block_rows = features // lax.axis_size("img")
    own_activated = lax.dynamic_slice_in_dim(
        all_activated, lax.axis_index("img") * block_rows, block_rows, axis=1
    )
    modulation_grad_out = jnp.einsum(
        "id,ikc->dkc", own_activated, all_grads, preferred_element_type=jnp.float32
    )
    modulation_bias_out = jnp.sum(all_grads.astype(jnp.float32), axis=0)
    bias_parts = [
        query_bias_grad,
        value_bias_grad,
        project_bias_grad,
        expand_bias_grad,
        contract_bias_grad,
    ]
    bias_total = sum_all(jnp.concatenate(bias_parts))
    bias_outs = []
    place = 0
    for part in bias_parts:
        bias_outs.append(bias_total[place : place + part.shape[0]])
        place += part.shape[0]
    (
        query_bias_out,
        value_bias_out,
        project_bias_out,
        expand_bias_out,
        contract_bias_out,
    ) = bias_outs
    return (
        block_output,
        input_grad,
        conditioning_grad,
        modulation_grad_out,
        modulation_bias_out,
        attend_out,
        query_bias_out,
        value_bias_out,
        project_out,
        project_bias_out,
        expand_out,
        expand_bias_out,
        contract_out,
        contract_bias_out,
    )


def solution(mesh):
    in_specs = (
        P(("img", "band"), None),
        P("img", None),
        P(("img", "band")),
        P(("img", "band")),
        P(("img", "band")),
        P(None, "band", None),
        P("band", None),
        P(),
        P(),
        P(),
        P(),
        P(),
        P(),
        P(),
        P(),
        P(),
        P(("img", "band"), None),
    )
    out_specs = (
        P(("img", "band"), None),
        P(("img", "band"), None),
        P("img", None),
        P("img", "band", None),
        P("band", None),
        P("img", "band"),
        P(),
        P(),
        P("img", "band"),
        P(),
        P("img", "band"),
        P(),
        P("img", "band"),
        P(),
    )

    return jax.shard_map(shards, mesh=mesh, in_specs=in_specs, out_specs=out_specs, check_vma=False)
```

```python
import functools
import math

import jax
import jax.numpy as jnp
from jax import lax
from jax.experimental import pallas as pl
from jax.sharding import PartitionSpec as P


HEADS = 16


def layer_norm(values):
    row_mean = jnp.mean(values, axis=-1, keepdims=True)
    centred = values - row_mean
    spread = jnp.mean(centred * centred, axis=-1, keepdims=True)
    return centred * lax.rsqrt(spread + 1e-06)


def gelu_tanh(values):
    return (
        0.5
        * values
        * (1.0 + jnp.tanh(0.7978845608028654 * (values + 0.044715 * values * values * values)))
    )


def swish_gate(values):
    return values / (1.0 + jnp.exp(-values))


ROW_PLACES, COL_PLACES = 32, 64


def position_pieces(features):
    quarter = features // 4
    frequency = jnp.exp(-math.log(10000.0) * jnp.arange(quarter, dtype=jnp.float32) / quarter)
    angle = jnp.arange(COL_PLACES, dtype=jnp.float32)[:, None] * frequency[None, :]
    waves = jnp.concatenate([jnp.sin(angle), jnp.cos(angle)], axis=1)
    pieces = []
    for _ in range(3):
        piece = lax.reduce_precision(waves, 8, 7)
        pieces.append(piece.astype(jnp.bfloat16))
        waves = waves - piece
    blank = jnp.zeros_like(pieces[0])
    return jnp.concatenate(
        [jnp.concatenate([piece, blank], axis=1) for piece in pieces]
        + [jnp.concatenate([blank, piece], axis=1)[:ROW_PLACES] for piece in pieces],
        axis=0,
    )


def position_table(rows_in, cols_in, pieces):
    spot = jnp.arange(pieces.shape[0])[None, :]
    col_spots = 3 * COL_PLACES
    chosen = jnp.where(
        spot < col_spots,
        spot % COL_PLACES == cols_in[:, None],
        (spot - col_spots) % ROW_PLACES == rows_in[:, None],
    )
    return jnp.dot(chosen.astype(jnp.bfloat16), pieces, preferred_element_type=jnp.float32)


def norm_modulate(values, shift_rows, scale_rows):
    return layer_norm(values) * (1.0 + scale_rows[:, None, :]) + shift_rows[:, None, :]


def swap_bit(value, bit):
    members = lax.axis_size("img")
    return lax.ppermute(value, "img", [(i, i ^ (1 << bit)) for i in range(members)])


def swap_band(value):
    return lax.ppermute(value, "band", [(0, 1), (1, 0)])


def swap(value, stage):
    return swap_band(value) if stage == "band" else swap_bit(value, stage)


def my_bit(stage):
    if stage == "band":
        return lax.axis_index("band")
    return (lax.axis_index("img") >> stage) & 1


def pick(choice, if_zero, if_one):
    return jnp.where(choice == 0, if_zero, if_one)


def image_bits():
    return lax.axis_size("img").bit_length() - 1


def attend_kernel(score_scale, q_ref, k_ref, v_ref, kx_ref, vx_ref, mask_ref, out_ref, log_ref):
    keys = jnp.concatenate([k_ref[0], kx_ref[0]], axis=1)
    values = jnp.concatenate([v_ref[0], vx_ref[0]], axis=1)
    scores = lax.dot_general(
        keys, q_ref[0], (((0,), (0,)), ((), ())), preferred_element_type=jnp.float32
    )
    scores = jnp.where(mask_ref[...] > 0, scores * score_scale, -1e30)
    top = jnp.max(scores, axis=0, keepdims=True)
    weights = jnp.exp(scores - top)
    total = jnp.sum(weights, axis=0, keepdims=True)
    probabilities = (weights * (1.0 / total)).astype(jnp.bfloat16)
    out_ref[0] = jnp.dot(values, probabilities, preferred_element_type=jnp.float32).astype(
        jnp.bfloat16
    )
    log_ref[0] = top + jnp.log(total)


def head_blocks(size, rows, heads):
    block = lambda base: pl.BlockSpec((1, size, rows), lambda h: (base * heads + h, 0, 0))
    return [block(0), block(1), block(2), block(0), block(1)]


def attend_forward(own, other, mask, score_scale):
    heads, (_, size, rows) = HEADS, own.shape
    columns = 2 * rows
    return pl.pallas_call(
        functools.partial(attend_kernel, score_scale),
        grid=(heads,),
        in_specs=head_blocks(size, rows, heads)
        + [pl.BlockSpec((columns, 1), lambda h: (0, 0))],
        out_specs=[
            pl.BlockSpec((1, size, rows), lambda h: (h, 0, 0)),
            pl.BlockSpec((1, 1, rows), lambda h: (h, 0, 0)),
        ],
        out_shape=[
            jax.ShapeDtypeStruct((heads, size, rows), jnp.bfloat16),
            jax.ShapeDtypeStruct((heads, 1, rows), jnp.float32),
        ],
        cost_estimate=pl.CostEstimate(
            flops=16 * heads * 128 * rows * columns,
            bytes_accessed=4 * heads * size * (rows + columns),
            transcendentals=heads * rows * columns,
        ),
    )(own, own, own, other, other, mask)


def attend_back_kernel(
    score_scale,
    q_ref,
    k_ref,
    v_ref,
    kx_ref,
    vx_ref,
    go_ref,
    log_ref,
    mask_ref,
    dq_ref,
    own_ref,
    other_ref,
):
    queries, grads = q_ref[0], go_ref[0]
    keys = jnp.concatenate([k_ref[0], kx_ref[0]], axis=1)
    values = jnp.concatenate([v_ref[0], vx_ref[0]], axis=1)
    rows = queries.shape[1]

    def outer(left, right):
        return lax.dot_general(
            left, right, (((0,), (0,)), ((), ())), preferred_element_type=jnp.float32
        )

    def across(left, right):
        return lax.dot_general(
            left, right, (((1,), (1,)), ((), ())), preferred_element_type=jnp.float32
        )

    scores = jnp.where(mask_ref[...] > 0, outer(keys, queries) * score_scale, -1e30)
    weights = jnp.exp(scores - log_ref[0])
    grad_weights = outer(values, grads)
    delta = jnp.sum(weights * grad_weights, axis=0, keepdims=True)
    grad_scores = (weights * (grad_weights - delta)).astype(jnp.bfloat16)
    grad_values = across(grads, weights.astype(jnp.bfloat16))
    grad_keys = across(queries, grad_scores) * score_scale
    for i, grad in enumerate((grad_keys, grad_values)):
        own_ref[i, 0] = grad[:, :rows]
        other_ref[i, 0] = grad[:, rows:].astype(other_ref.dtype)
    dq_ref[0] = (
        jnp.dot(keys, grad_scores, preferred_element_type=jnp.float32) * score_scale
    ).astype(dq_ref.dtype)


def attend_backward(own, other, grads, log_total, mask, score_scale):
    heads, (_, size, rows) = HEADS, own.shape
    columns = 2 * rows
    single = pl.BlockSpec((1, size, rows), lambda h: (h, 0, 0))
    double = pl.BlockSpec((2, 1, size, rows), lambda h: (0, h, 0, 0))
    return pl.pallas_call(
        functools.partial(attend_back_kernel, score_scale),
        grid=(heads,),
        in_specs=head_blocks(size, rows, heads)
        + [
            single,
            pl.BlockSpec((1, 1, rows), lambda h: (h, 0, 0)),
            pl.BlockSpec((columns, 1), lambda h: (0, 0)),
        ],
        out_specs=[single, double, double],
        out_shape=[
            jax.ShapeDtypeStruct((heads, size, rows), jnp.bfloat16),
            jax.ShapeDtypeStruct((2, heads, size, rows), jnp.float32),
            jax.ShapeDtypeStruct((2, heads, size, rows), jnp.bfloat16),
        ],
        cost_estimate=pl.CostEstimate(
            flops=30 * heads * 128 * rows * columns,
            bytes_accessed=8 * heads * size * (rows + columns),
            transcendentals=heads * rows * columns,
        ),
    )(own, own, own, other, other, grads, log_total, mask)


def column_tile(width):
    return 384 if width % 384 == 0 else width


def project_kernel(rows_ref, weight_ref, bias_ref, out_ref):
    flat = jnp.dot(rows_ref[...], weight_ref[...], preferred_element_type=jnp.float32)
    out_ref[...] = (flat + bias_ref[...].astype(jnp.float32)).T.astype(out_ref.dtype)


def project_rows(rows, weight, bias, skip):
    depth = weight.shape[0]
    width = weight.shape[1] - skip
    tile = column_tile(depth)
    first = skip // tile
    return pl.pallas_call(
        project_kernel,
        grid=(width // tile,),
        in_specs=[
            pl.BlockSpec(rows.shape, lambda n: (0, 0)),
            pl.BlockSpec((depth, tile), lambda n: (0, n + first)),
            pl.BlockSpec((1, tile), lambda n: (0, n + first)),
        ],
        out_specs=pl.BlockSpec((tile, rows.shape[0]), lambda n: (n, 0)),
        out_shape=jax.ShapeDtypeStruct((width, rows.shape[0]), jnp.bfloat16),
        cost_estimate=pl.CostEstimate(
            flops=2 * rows.shape[0] * depth * width,
            bytes_accessed=2 * depth * width,
            transcendentals=0,
        ),
    )(rows, weight, bias)


def dense_kernel(rows_ref, weight_ref, bias_ref, out_ref):
    flat = jnp.dot(rows_ref[...], weight_ref[...], preferred_element_type=jnp.float32)
    out_ref[...] = flat + bias_ref[...].astype(jnp.float32)


def dense(rows, weight, bias):
    depth, width = weight.shape
    tile = column_tile(width)
    return pl.pallas_call(
        dense_kernel,
        grid=(width // tile,),
        in_specs=[
            pl.BlockSpec(rows.shape, lambda n: (0, 0)),
            pl.BlockSpec((depth, tile), lambda n: (0, n)),
            pl.BlockSpec((1, tile), lambda n: (0, n)),
        ],
        out_specs=pl.BlockSpec((rows.shape[0], tile), lambda n: (0, n)),
        out_shape=jax.ShapeDtypeStruct((rows.shape[0], width), jnp.float32),
        cost_estimate=pl.CostEstimate(
            flops=2 * rows.shape[0] * depth * width,
            bytes_accessed=2 * depth * width,
            transcendentals=0,
        ),
    )(rows, weight, bias[None, :])


def dense_back_kernel(grad_ref, weight_ref, out_ref):
    flat = jnp.dot(weight_ref[...], grad_ref[...], preferred_element_type=jnp.float32)
    out_ref[...] = flat.T


def dense_back(grad, weight):
    width, depth = weight.shape
    tile = column_tile(width)
    return pl.pallas_call(
        dense_back_kernel,
        grid=(width // tile,),
        in_specs=[
            pl.BlockSpec(grad.shape, lambda n: (0, 0)),
            pl.BlockSpec((tile, depth), lambda n: (n, 0)),
        ],
        out_specs=pl.BlockSpec((grad.shape[1], tile), lambda n: (0, n)),
        out_shape=jax.ShapeDtypeStruct((grad.shape[1], width), jnp.float32),
        cost_estimate=pl.CostEstimate(
            flops=2 * grad.shape[1] * depth * width,
            bytes_accessed=2 * depth * width,
            transcendentals=0,
        ),
    )(grad, weight)


def product_kernel(
    left_axis, right_axis, columns, orders, per_step, left_ref, left_far, right_ref,
    right_far, *out_refs
):
    contract = (((left_axis,), (right_axis,)), ((), ()))
    near = lax.dot_general(
        left_ref[...], right_ref[...], contract, preferred_element_type=jnp.float32
    )
    far = lax.dot_general(
        left_far[...], right_far[...], contract, preferred_element_type=jnp.float32
    )
    total = (near + far).astype(jnp.bfloat16)
    padded = total.shape[1] // 2
    chunk = total.shape[0] // per_step
    part = chunk // len(orders)

    def piece(band, index, i):
        start = index * chunk + i * part
        return total[start : start + part, band * padded : band * padded + columns]

    for i, order in enumerate(orders):
        going_ref, staying_ref = out_refs[2 * i], out_refs[2 * i + 1]
        if order[0] == "band":
            for index in range(per_step):
                going_ref[index] = piece(0, index, i)
                staying_ref[index] = piece(1, index, i)
        else:
            side = (lax.axis_index("img") >> order[0]) & 1
            step = 1 << (order[0] - 1)
            slot = 0
            for index in range(per_step):
                if index & step:
                    continue
                for band in range(2):
                    first, second = piece(band, index, i), piece(band, index | step, i)
                    going_ref[band, slot] = jnp.where(side == 0, second, first)
                    staying_ref[band, slot] = jnp.where(side == 0, first, second)
                slot += 1


def row_product(left, left_far, right, right_far, left_axis, right_axis, columns, orders):
    depth, width = left.shape[left_axis], left.shape[1 - left_axis]
    bits = image_bits()
    chunks = 1 << (bits - 1)
    tile = width // 4 if width > 2 * right.shape[1 - right_axis] else width
    per_step = chunks * tile // width
    part = width // chunks // len(orders)
    left_block = (
        pl.BlockSpec((depth, tile), lambda k: (0, k))
        if left_axis == 0
        else pl.BlockSpec((tile, depth), lambda k: (k, 0))
    )
    right_block = pl.BlockSpec(right.shape, lambda k: (0, 0))
    out_specs, out_shape = [], []
    for order in orders:
        if order[0] == "band":
            shape, block = (chunks, part, columns), (per_step, part, columns)
            spec = pl.BlockSpec(block, lambda k: (k, 0, 0))
        else:
            shape = (2, chunks // 2, part, columns)
            spec = pl.BlockSpec((2, per_step // 2, part, columns), lambda k: (0, k, 0, 0))
        out_specs += [spec, spec]
        out_shape += [jax.ShapeDtypeStruct(shape, jnp.bfloat16)] * 2
    outs = pl.pallas_call(
        functools.partial(
            product_kernel, left_axis, right_axis, columns, orders, per_step
        ),
        grid=(width // tile,),
        in_specs=[left_block, left_block, right_block, right_block],
        out_specs=out_specs,
        out_shape=out_shape,
        cost_estimate=pl.CostEstimate(
            flops=8 * depth * width * columns,
            bytes_accessed=8 * depth * (width + columns) + 4 * width * columns,
            transcendentals=0,
        ),
    )(left, left_far, right, right_far)
    halves = []
    for i, order in enumerate(orders):
        left_bits = ["band"] + list(range(bits - 1, 0, -1))
        left_bits.remove(order[0])
        shape = (2,) * len(left_bits) + (part, columns)
        halves.append((outs[2 * i].reshape(shape), outs[2 * i + 1].reshape(shape)))
    return halves


def core_columns(values, axis, core, band):
    quarter = values.shape[axis] // 4
    pieces = [lax.slice_in_dim(values, i * quarter, (i + 1) * quarter, axis=axis) for i in range(4)]
    return pick(
        band, pick(core, pieces[0], pieces[1]), pick(core, pieces[2], pieces[3])
    )


def halved_kernel(columns, part, left_ref, left_far, right_ref, right_far, going_ref, staying_ref):
    core = lax.axis_index("img") & 1
    chips = left_ref.shape[1] // (2 * part)

    def own_rows(ref):
        rows = ref[...].T
        pieces = [rows[i * part : (i + 1) * part] for i in range(2 * chips)]
        return jnp.concatenate(
            [jnp.where(core == 0, pieces[2 * i], pieces[2 * i + 1]) for i in range(chips)], axis=0
        )

    near = jnp.dot(own_rows(left_ref), right_ref[...], preferred_element_type=jnp.float32)
    far = jnp.dot(own_rows(left_far), right_far[...], preferred_element_type=jnp.float32)
    total = (near + far).astype(jnp.bfloat16)
    padded = total.shape[1] // 2
    side = (lax.axis_index("img") >> 1) & 1
    for i in range(2):
        pieces = [
            total[x * part : (x + 1) * part, i * padded : i * padded + columns]
            for x in range(chips)
        ]
        for x in range(chips // 2):
            first, second = pieces[2 * x], pieces[2 * x + 1]
            going_ref[i, x] = jnp.where(side == 0, second, first)
            staying_ref[i, x] = jnp.where(side == 0, first, second)


def halved_product(left, right):
    depth, width = left.shape
    bits = image_bits()
    chips = 1 << (bits - 1)
    band = my_bit("band")
    columns = right.shape[1] // 2
    halves = [right[:, :columns], right[:, columns:]]
    right = jnp.concatenate(
        [
            jnp.pad(pick(band, *pair), [(0, 0), (0, -columns % 128)])
            for pair in (halves[::-1], halves)
        ],
        axis=1,
    )
    right_far = swap_bit(right, 0)
    tile, part = width // 4, width // chips // 2
    left_block = pl.BlockSpec((depth, tile), lambda k: (0, k))
    right_block = pl.BlockSpec(right.shape, lambda k: (0, 0))
    out_block = pl.BlockSpec((2, chips // 8, part, columns), lambda k: (0, k, 0, 0))
    out_shape = jax.ShapeDtypeStruct((2, chips // 2, part, columns), jnp.bfloat16)
    going, staying = pl.pallas_call(
        functools.partial(halved_kernel, columns, part),
        grid=(4,),
        in_specs=[left_block, left_block, right_block, right_block],
        out_specs=[out_block, out_block],
        out_shape=[out_shape, out_shape],
        cost_estimate=pl.CostEstimate(
            flops=4 * depth * width * columns,
            bytes_accessed=8 * depth * (width + columns) + 4 * width * columns,
            transcendentals=0,
        ),
    )(left, swap_bit(left, 0), right, right_far)
    shape = (2,) * (bits - 1) + (part, columns)
    return going.reshape(shape), staying.reshape(shape)


def chip_product(left, right, orders, left_axis=0, right_axis=0):
    core, band = my_bit(0), my_bit("band")
    axis = 1 - right_axis
    columns = right.shape[axis] // 4
    edges = [(0, 0), (0, 0)]
    edges[axis] = (0, -columns % 128)

    def chosen(which):
        return jnp.concatenate(
            [jnp.pad(core_columns(right, axis, which, b), edges) for b in (1 - band, band)],
            axis=axis,
        )

    left_far, right_far = swap_bit(left, 0), swap_bit(chosen(1 - core), 0)
    return row_product(
        left, left_far, chosen(core), right_far, left_axis, right_axis, columns, orders
    )


def scatter_sum(halves, orders):
    core = my_bit(0)
    totals = [scatter_part(*pair, order) for pair, order in zip(halves, orders)]
    total = jnp.concatenate(totals, axis=0) if len(totals) > 1 else totals[0]
    rows = total.shape[0] // 2
    low, high = total[:rows], total[rows:]
    here, there = pick(core, low, high), swap_bit(pick(core, high, low), 0)
    return pick(
        core,
        jnp.concatenate([here, there], axis=1),
        jnp.concatenate([there, here], axis=1),
    )


def scatter_part(going, staying, order):
    alive = ["band"] + list(range(image_bits() - 1, 0, -1))
    for stage in order:
        axis = alive.index(stage)
        alive.remove(stage)
        if stage != order[0]:
            first = lax.index_in_dim(block, 0, axis, keepdims=False)
            second = lax.index_in_dim(block, 1, axis, keepdims=False)
            if stage == "band":
                going, staying = first, second
            else:
                side = my_bit(stage)
                going, staying = pick(side, second, first), pick(side, first, second)
        arrived = swap(going, stage)
        block = staying.astype(jnp.float32) + arrived.astype(jnp.float32)
        if stage != order[-1]:
            block = block.astype(jnp.bfloat16)
    return block


def sum_all(value):
    for stage in ["band"] + list(range(image_bits())):
        value = value + swap(value, stage)
    return value


def gather_images(value):
    for stage in range(image_bits()):
        other = swap_bit(value, stage)
        side = my_bit(stage)
        value = jnp.concatenate([pick(side, value, other), pick(side, other, value)], axis=0)
    return value


def shards(
    block_input,
    conditioning,
    patch_valid,
    pos_rows,
    pos_cols,
    modulation_weight,
    modulation_bias,
    attend_weight,
    query_bias,
    value_bias,
    project_weight,
    project_bias,
    expand_weight,
    expand_bias,
    contract_weight,
    contract_bias,
    out_cotangent,
):
    slot_count, features = block_input.shape
    image_count = conditioning.shape[0]
    per_image = slot_count // image_count
    head_count = HEADS
    rest = list(range(3, image_bits()))
    expand_order = [2, 1, "band"] + rest
    contract_order = [1, 2, "band"] + rest
    project_order = ["band", 2, 1] + rest
    attend_orders = [[1, "band", 2] + rest, ["band", 2, 1] + rest, [2, 1, "band"] + rest]
    head_size = features // head_count
    score_scale = 1.0 / math.sqrt(head_size)
    valid_rows = patch_valid.astype(jnp.float32)
    band = lax.axis_index("band")
    other_places = swap_band(jnp.stack([pos_rows, pos_cols, patch_valid]))
    sent_input, other_places = lax.optimization_barrier((block_input, other_places))
    other_input = swap_band(sent_input)
    pieces = position_pieces(features)
    pos_table = position_table(pos_rows, pos_cols, pieces)
    other_table = position_table(other_places[0], other_places[1], pieces)
    hidden = block_input.astype(jnp.float32) + pos_table
    shaped = hidden.reshape(image_count, per_image, features)
    cond_float = conditioning.astype(jnp.float32)
    swish_value, swish_back = jax.vjp(swish_gate, cond_float)
    activated = swish_value.astype(jnp.bfloat16)
    modulation_half = jnp.einsum(
        "id,dkc->ikc", activated, modulation_weight, preferred_element_type=jnp.float32
    ) + modulation_bias.astype(jnp.float32)
    modulation_other = swap_band(modulation_half)
    modulation = jnp.concatenate(
        [
            pick(band, modulation_half, modulation_other),
            pick(band, modulation_other, modulation_half),
        ],
        axis=1,
    )
    shift_one, scale_one, gate_one = (modulation[:, 0], modulation[:, 1], modulation[:, 2])
    shift_two, scale_two, gate_two = (modulation[:, 3], modulation[:, 4], modulation[:, 5])
    first_mod, first_back = jax.vjp(norm_modulate, shaped, shift_one, scale_one)
    first_low = first_mod.astype(jnp.bfloat16).reshape(slot_count, features)
    input_bias = jnp.concatenate([query_bias, jnp.zeros_like(query_bias), value_bias])[None, :]

    def project_heads(rows, skip):
        flat = project_rows(rows, attend_weight, input_bias, skip)
        return flat.reshape(-1, head_size, slot_count)

    own_heads, other_input = lax.optimization_barrier(
        (project_heads(first_low, 0), other_input)
    )
    other_shaped = (other_input.astype(jnp.float32) + other_table).reshape(
        image_count, per_image, features
    )
    other_low = (
        norm_modulate(other_shaped, shift_one, scale_one)
        .astype(jnp.bfloat16)
        .reshape(slot_count, features)
    )
    other_heads = project_heads(other_low, features)
    key_mask = jnp.concatenate([patch_valid, other_places[2]]).astype(jnp.float32)[:, None]
    mixed_heads, log_total = attend_forward(own_heads, other_heads, key_mask, score_scale)
    mixed_low = mixed_heads.reshape(features, slot_count)
    branch = jnp.einsum(
        "et,ed->td", mixed_low, project_weight, preferred_element_type=jnp.float32
    ) + project_bias.astype(jnp.float32)
    branch_rows = branch.reshape(image_count, per_image, features)
    middle = shaped + gate_one[:, None, :] * branch_rows
    second_mod, second_back = jax.vjp(norm_modulate, middle, shift_two, scale_two)
    second_low = second_mod.astype(jnp.bfloat16).reshape(slot_count, features)
    expanded = jnp.dot(
        second_low, expand_weight, preferred_element_type=jnp.float32
    ) + expand_bias.astype(jnp.float32)
    activation, gelu_back = jax.vjp(gelu_tanh, expanded)
    activation_low = activation.astype(jnp.bfloat16)
    mlp_out = dense(activation_low, contract_weight, contract_bias)
    mlp_rows = mlp_out.reshape(image_count, per_image, features)
    result = middle + gate_two[:, None, :] * mlp_rows
    block_output = result.reshape(slot_count, features).astype(jnp.bfloat16)
    upstream = (out_cotangent.astype(jnp.float32) * valid_rows[:, None]).reshape(
        image_count, per_image, features
    )
    grad_gate_two = jnp.sum(upstream * mlp_rows, axis=1)
    grad_mlp = (gate_two[:, None, :] * upstream).reshape(slot_count, features).astype(jnp.bfloat16)
    contract_chip = halved_product(activation_low, grad_mlp)
    contract_bias_grad = jnp.sum(grad_mlp.astype(jnp.float32), axis=0)
    grad_activation = jnp.einsum(
        "td,fd->tf", grad_mlp, contract_weight, preferred_element_type=jnp.float32
    )
    grad_expanded = gelu_back(grad_activation)[0].astype(jnp.bfloat16)
    expand_chip = chip_product(second_low, grad_expanded, [expand_order])
    expand_bias_grad = jnp.sum(grad_expanded.astype(jnp.float32), axis=0)
    grad_second = jnp.einsum(
        "tf,df->td", grad_expanded, expand_weight, preferred_element_type=jnp.float32
    )
    grad_norm_two, grad_shift_two, grad_scale_two = second_back(
        grad_second.reshape(image_count, per_image, features)
    )
    grad_middle = upstream + grad_norm_two
    grad_gate_one = jnp.sum(grad_middle * branch_rows, axis=1)
    grad_branch = (
        (gate_one[:, None, :] * grad_middle).reshape(slot_count, features).astype(jnp.bfloat16)
    )
    grad_branch, contract_chip, expand_chip = lax.optimization_barrier(
        (grad_branch, contract_chip, expand_chip)
    )
    contract_out = scatter_part(*contract_chip, contract_order)
    expand_out = scatter_sum(expand_chip, [expand_order])
    project_chip = chip_product(mixed_low, grad_branch, [project_order], left_axis=1)
    project_bias_grad = jnp.sum(grad_branch.astype(jnp.float32), axis=0)
    grad_mixed = jnp.einsum(
        "td,ed->et", grad_branch, project_weight, preferred_element_type=jnp.float32
    ).astype(jnp.bfloat16)
    grad_query, grad_pair, grad_pair_other = attend_backward(
        own_heads,
        other_heads,
        grad_mixed.reshape(head_count, head_size, slot_count),
        log_total,
        key_mask,
        score_scale,
    )
    grad_pair_far = swap_band(grad_pair_other)
    grad_pair_far, project_chip = lax.optimization_barrier((grad_pair_far, project_chip))
    project_out = scatter_sum(project_chip, [project_order])
    grad_pair = grad_pair + grad_pair_far.astype(jnp.float32)
    grad_qkv = jnp.concatenate(
        [
            grad_query.reshape(features, slot_count),
            grad_pair.astype(jnp.bfloat16).reshape(2 * features, slot_count),
        ],
        axis=0,
    )
    attend_chip = chip_product(first_low, grad_qkv, attend_orders, right_axis=1)
    query_bias_grad = jnp.sum(grad_qkv[:features].astype(jnp.float32), axis=1)
    value_bias_grad = jnp.sum(grad_qkv[2 * features :].astype(jnp.float32), axis=1)
    grad_first = dense_back(grad_qkv, attend_weight)
    grad_first, attend_chip = lax.optimization_barrier((grad_first, attend_chip))
    attend_out = scatter_sum(attend_chip, attend_orders)
    grad_norm_one, grad_shift_one, grad_scale_one = first_back(
        grad_first.reshape(image_count, per_image, features)
    )
    input_grad = (grad_middle + grad_norm_one).reshape(slot_count, features)
    grad_modulation = jnp.stack(
        [
            grad_shift_one,
            grad_scale_one,
            grad_gate_one,
            grad_shift_two,
            grad_scale_two,
            grad_gate_two,
        ],
        axis=1,
    )
    grad_halves = grad_modulation.reshape(image_count, 2, -1, features)
    grad_half_far = swap_band(pick(band, grad_halves[:, 1], grad_halves[:, 0]))
    modulation_grad_half = (
        pick(band, grad_halves[:, 0], grad_halves[:, 1]) + grad_half_far
    ).astype(jnp.bfloat16)
    activated_grad_part = jnp.einsum(
        "ikc,dkc->id", modulation_grad_half, modulation_weight, preferred_element_type=jnp.float32
    )
    conditioning_grad = swish_back(activated_grad_part + swap_band(activated_grad_part))[0]
    all_grads = gather_images(modulation_grad_half)
    all_activated = gather_images(activated)
    block_rows = features // lax.axis_size("img")
    own_activated = lax.dynamic_slice_in_dim(
        all_activated, lax.axis_index("img") * block_rows, block_rows, axis=1
    )
    modulation_grad_out = jnp.einsum(
        "id,ikc->dkc", own_activated, all_grads, preferred_element_type=jnp.float32
    )
    modulation_bias_out = jnp.sum(all_grads.astype(jnp.float32), axis=0)
    bias_parts = [
        query_bias_grad,
        value_bias_grad,
        project_bias_grad,
        expand_bias_grad,
        contract_bias_grad,
    ]
    bias_total = sum_all(jnp.concatenate(bias_parts))
    bias_outs = []
    place = 0
    for part in bias_parts:
        bias_outs.append(bias_total[place : place + part.shape[0]])
        place += part.shape[0]
    (
        query_bias_out,
        value_bias_out,
        project_bias_out,
        expand_bias_out,
        contract_bias_out,
    ) = bias_outs
    return (
        block_output,
        input_grad,
        conditioning_grad,
        modulation_grad_out,
        modulation_bias_out,
        attend_out,
        query_bias_out,
        value_bias_out,
        project_out,
        project_bias_out,
        expand_out,
        expand_bias_out,
        contract_out,
        contract_bias_out,
    )


def solution(mesh):
    in_specs = (
        P(("img", "band"), None),
        P("img", None),
        P(("img", "band")),
        P(("img", "band")),
        P(("img", "band")),
        P(None, "band", None),
        P("band", None),
        P(),
        P(),
        P(),
        P(),
        P(),
        P(),
        P(),
        P(),
        P(),
        P(("img", "band"), None),
    )
    out_specs = (
        P(("img", "band"), None),
        P(("img", "band"), None),
        P("img", None),
        P("img", "band", None),
        P("band", None),
        P("img", "band"),
        P(),
        P(),
        P("img", "band"),
        P(),
        P("img", "band"),
        P(),
        P("img", "band"),
        P(),
    )

    return jax.shard_map(shards, mesh=mesh, in_specs=in_specs, out_specs=out_specs, check_vma=False)
```
